512 devices in a mesh: expert: 8 (over x, core), dp: 64 (over z, y).
Axes of the slice: x: 4, y: 4, z: 16, core: 2. Of those that a mesh axis runs over, the one named last changes fastest.
Arguments:
- grads: bfloat16 [8, 64, 128, 6144], P('expert', 'dp'), may hold values from -16 to 16
- master: float32 [8, 128, 6144], P('expert', 'dp'), may hold values from -0.0625 to 0.0625
- first_moment: float32 [8, 128, 6144], P('expert', 'dp'), may hold values from -0.0029296875 to 0.0029296875
- second_moment: float32 [8, 128, 6144], P('expert', 'dp'), may hold values from 1e-08 to 1e-07
Outputs:
- new_master: float32 [8, 128, 6144], P('expert', 'dp')
- new_first: float32 [8, 128, 6144], P('expert', 'dp')
- new_second: float32 [8, 128, 6144], P('expert', 'dp')
- direction: float32 [8, 128, 6144], P('expert', 'dp')
- new_weights: bfloat16 [8, 128, 6144], P('expert')
The draws below stay inside these ranges and needn't reach their ends.
All inputs are finite; a program needn't handle non-finite values.
Results may differ from the reference program's by a relative error of at most 0.0004.
Values may be sent and summed in bfloat16 or wider, within the bound.
A program may use at most 64 MiB of HBM per device.

```python
import math
import jax
import jax.numpy as jnp
from jax import lax

D = 6144
ROWS = 128
STEP = 10
EXPERTS = 8
N_DP = 64


def draw_grads(key, part):
    key_common = jax.random.fold_in(key, 11)
    key_scale = jax.random.fold_in(key, 12)
    key_noise = jax.random.fold_in(key, 13)
    key_pairs = jax.random.fold_in(key, 14)
    rows_per = ROWS // N_DP
    row_scale = jnp.exp(jax.random.uniform(key_scale, (EXPERTS, 1, ROWS, 1), jnp.float32, math.log(0.5), math.log(2.0)))
    pairing = jax.random.permutation(key_pairs, N_DP)
    owner = jnp.arange(ROWS, dtype=jnp.int32) // rows_per
    spike = jnp.where(owner[None, :] == pairing[:, None], 4.0, 1.0).astype(jnp.float32)
    spike = spike.reshape(1, N_DP, ROWS, 1)
    common = 0.25 * row_scale * jax.random.truncated_normal(key_common, -4.0, 4.0, (EXPERTS, 1, ROWS, D), jnp.float32)
    noise = jax.random.truncated_normal(key_noise, -3.0, 3.0, (EXPERTS, N_DP, ROWS, D), jnp.float32)
    return (common + spike * noise).astype(jnp.bfloat16)


def block_levels(key, extent, cuts, least, largest):
    gain = 1.0
    for axis_at, parts in cuts:
        steps = jax.random.uniform(jax.random.fold_in(jax.random.fold_in(key, 6), axis_at), (parts,), jnp.float32, least / len(cuts), largest / len(cuts))
        gain = gain * jnp.repeat(jnp.exp(steps), extent[axis_at] // parts).reshape((-1,) + (1,) * (len(extent) - 1 - axis_at))
    return gain


def normal_values(stream_key, extent, deviation, most, shards=(), held_as=jnp.bfloat16):
    result = deviation * jax.random.normal(stream_key, extent, jnp.float32)
    if shards:
        result = result * block_levels(stream_key, extent, shards, -0.22, 0.18)
    return jnp.clip(result, -most, most).astype(held_as)


def setup_inputs(seed: int = 0) -> dict:
    seeds = jax.random.split(jax.random.key(seed), 5)
    return {
        "grads": draw_grads(jax.random.fold_in(seeds[4], 71), 0),
        "master": normal_values(seeds[1], (EXPERTS, ROWS, D), 0.004, 0.0625, ((0, 8), (1, 64)), jnp.float32),
        "first_moment": normal_values(seeds[2], (EXPERTS, ROWS, D), 0.0002, 0.0029296875, ((0, 8), (1, 64)), jnp.float32),
        "second_moment": jnp.clip(jnp.exp(math.log(1.0000000116860974e-07) - 2.3025851 * jax.random.uniform(seeds[3], (EXPERTS, ROWS, D), jnp.float32) ** block_levels(seeds[3], (EXPERTS, ROWS, D), ((0, 8), (1, 64)), -0.2, 0.2)), 9.99999993922529e-09, 1.0000000116860974e-07),
    }


def reference(grads, master, first_moment, second_moment):

    def add_one(index, total):
        piece = lax.dynamic_index_in_dim(grads, index, 1, keepdims=False)
        return total + piece.astype(jnp.float32)
    summed = lax.fori_loop(0, grads.shape[1], add_one, jnp.zeros(master.shape, jnp.float32))
    norm = jnp.sqrt(jnp.sum(summed * summed))
    clip = 1.0 / jnp.maximum(norm, 1.0)
    clipped = clip * summed
    new_first = 0.9 * first_moment + 0.1 * clipped
    new_second = 0.95 * second_moment + 0.05 * (clipped * clipped)
    first_fix = 1.0 - 0.9 ** STEP
    second_fix = 1.0 - 0.95 ** STEP
    direction = new_first / first_fix / (jnp.sqrt(new_second / second_fix) + 1e-08)
    new_master = master - 0.001 * (direction + 0.1 * master)
    new_weights = new_master.astype(jnp.bfloat16)
    return (new_master, new_first, new_second, direction, new_weights)
```

```python
import functools

import jax
import jax.numpy as jnp
from jax import lax
from jax.experimental import pallas as pl
from jax.experimental.pallas import tpu as pltpu
from jax.sharding import PartitionSpec as P

STEP = 10
NY = 4
AG_STRIDE = 2
MESH = pl.DeviceIdType.MESH


def adam(clip, summed, master, first, second):
    clipped = clip * summed
    new_first = 0.9 * first + 0.1 * clipped
    new_second = 0.95 * second + 0.05 * (clipped * clipped)
    first_fix = 1.0 - 0.9**STEP
    second_fix = 1.0 - 0.95**STEP
    direction = new_first / first_fix / (jnp.sqrt(new_second / second_fix) + 1e-08)
    new_master = master - 0.001 * (direction + 0.1 * master)
    return new_master, new_first, new_second, direction


def kernel(
    n_e, nz, quarter,
    g_hbm, master_ref, first_ref, second_ref,
    o_master, o_first, o_second, o_direction, w_ref,
    g, own_q, yin, rin, zin, zout, total_q, s_out, s_in, t_in, norm_out, n1, norm2_out, n2,
    load_sem, own_sem, y_ssem, y_rsem, r_ssem, r_rsem, z_ssem, z_rsem,
    x_ssem, x_rsem, n1_ssem, n1_rsem, n2_ssem, n2_rsem,
    az_ssem, az_rsem, ay_ssem, ay_rsem, ar_ssem, ar_rsem,
):
    half = quarter // 2
    hz = nz // 2
    e = lax.axis_index("expert")
    d = lax.axis_index("dp")
    z = d // NY
    y = d % NY

    def at(zz, yy):
        return (e, ((zz + nz) % nz) * NY + (yy + NY) % NY)

    def columns(q):
        return pl.ds(pl.multiple_of(q * quarter, 128), quarter)

    loads = []
    for i in range(NY):
        q = (y + 1 + i) % NY
        dst = g.at[:, :, pl.ds(i * quarter, quarter)] if i < NY - 1 else own_q
        copy = pltpu.make_async_copy(g_hbm.at[:, :, columns(q)], dst, load_sem.at[i])
        copy.start()
        loads.append(copy)

    barrier = pltpu.get_barrier_semaphore()
    for dz in (1, -1):
        pl.semaphore_signal(barrier, inc=1, device_id=at(z + dz, y), device_id_type=MESH)

    def greet(i, carry):
        i = i + 1
        ee = (e + i // NY) % n_e
        yy = (y + i % NY) % NY
        pl.semaphore_signal(barrier, inc=1, device_id=(ee, z * NY + yy), device_id_type=MESH)
        return carry

    lax.fori_loop(0, n_e * NY - 1, greet, 0)
    pl.semaphore_wait(barrier, n_e * NY + 1)
    for copy in loads:
        copy.wait()

    def tile(j):
        i = (j + 1) // 2
        sign = 2 * (j % 2) - 1
        return (z + 2 * nz + sign * (hz - i)) % nz

    def y_copy(way, j):
        src = g.at[tile(j), :, pl.ds(way * 3 * half, 3 * half)]
        return pltpu.make_async_remote_copy(
            src_ref=src, dst_ref=yin.at[way, j], send_sem=y_ssem.at[way, j], recv_sem=y_rsem.at[way, j],
            device_id=at(z, y + 1 - 2 * way), device_id_type=MESH)

    def relay(way, j):
        src = yin.at[way, j, :, pl.ds(2 * half if way == 0 else 0, half)]
        return pltpu.make_async_remote_copy(
            src_ref=src, dst_ref=rin.at[way, j], send_sem=r_ssem.at[way, j], recv_sem=r_rsem.at[way, j],
            device_id=at(z, y + 1 - 2 * way), device_id_type=MESH)

    def z_copy(way, i, h):
        return pltpu.make_async_remote_copy(
            src_ref=zout.at[way, i, h], dst_ref=zin.at[way, i + 1, h],
            send_sem=z_ssem.at[way, i, h], recv_sem=z_rsem.at[way, i + 1, h],
            device_id=at(z + 1 - 2 * way, y), device_id_type=MESH)

    def arrive(j):
        for way in (0, 1):
            y_copy(way, j).wait_recv()
            relay(way, j).start()

    def y_start(j):
        for way in (0, 1):
            y_copy(way, j).start()

    def y_sum(j, h):
        cols = pl.ds(h * half, half)
        own = own_q[tile(j), :, cols].astype(jnp.float32)
        left = yin[0, j, :, cols].astype(jnp.float32)
        right = yin[1, j, :, pl.ds(half + h * half, half)].astype(jnp.float32)
        far = rin[h, j].astype(jnp.float32)
        return (own + left) + (right + far)

    def z_step(i, ways, begins):
        for h in (0, 1):
            for way in ways:
                j = 0 if isinstance(i, int) and i == 0 else 2 * i - 1 + way
                relay(h, j).wait_recv()
                value = y_sum(j, h)
                if not begins[way]:
                    z_copy(way, i - 1, h).wait_recv()
                    value = value + zin[way, i, h]
                zout[way, i, h] = value
                z_copy(way, i, h).start()

    for j in (0, 1, 2):
        y_start(j)
    arrive(0)
    for j in (3, 4):
        if j < nz:
            y_start(j)
    arrive(1)
    arrive(2)
    for j in (5, 6):
        if j < nz:
            y_start(j)
    z_step(0, (0,), (True, True))
    for j in (3, 4):
        if j < nz:
            arrive(j)
    for j in (7, 8):
        if j < nz:
            y_start(j)
    z_step(1, (0, 1), (False, True))

    def middle(i, carry):
        arrive(2 * i + 1)
        pl.when(2 * i + 2 < nz)(lambda: arrive(2 * i + 2))
        pl.when(2 * i + 5 < nz)(lambda: y_start(2 * i + 5))
        pl.when(2 * i + 6 < nz)(lambda: y_start(2 * i + 6))
        z_step(i, (0, 1), (False, False))
        return carry

    lax.fori_loop(2, hz, middle, 0)

    squares = jnp.zeros((8, half), jnp.float32)
    for h in (0, 1):
        relay(h, nz - 1).wait_recv()
        value = y_sum(nz - 1, h)
        for way in (0, 1):
            z_copy(way, hz - 1, h).wait_recv()
            value = value + zin[way, hz, h]
        total_q[:, pl.ds(h * half, half)] = value
        squares = squares + value * value

    norm_out[...] = jnp.sum(jnp.sum(squares.reshape(8, half // 128, 128), axis=1), axis=0, keepdims=True)
    mine = e * NY + y
    n1[mine] = norm_out[...]

    def n1_copy(i):
        ee = (e + i // NY) % n_e
        yy = (y + i % NY) % NY
        return pltpu.make_async_remote_copy(
            src_ref=norm_out, dst_ref=n1.at[mine], send_sem=n1_ssem.at[i], recv_sem=n1_rsem.at[i],
            device_id=(ee, z * NY + yy), device_id_type=MESH)

    lax.fori_loop(1, n_e * NY, lambda i, c: (n1_copy(i).start(), c)[1], 0)

    for k in range(NY):
        s_out[k] = total_q[pl.ds(2 * k, 2), :]

    def x_copies(i):
        yy = (y + i) % NY
        copies = [pltpu.make_async_remote_copy(
            src_ref=s_out.at[yy], dst_ref=s_in.at[y], send_sem=x_ssem.at[0, i], recv_sem=x_rsem.at[0, i],
            device_id=at(z, yy), device_id_type=MESH)]
        for a, ref in enumerate((master_ref, first_ref, second_ref)):
            copies.append(pltpu.make_async_remote_copy(
                src_ref=ref.at[:, columns(yy)], dst_ref=t_in.at[a, y],
                send_sem=x_ssem.at[a + 1, i], recv_sem=x_rsem.at[a + 1, i],
                device_id=at(z, yy), device_id_type=MESH))
        return copies

    for i in range(1, NY):
        for copy in x_copies(i):
            copy.start()
    s_in[y] = s_out[y]
    for a, ref in enumerate((master_ref, first_ref, second_ref)):
        t_in[a, y] = ref[:, columns(y)]

    lax.fori_loop(1, n_e * NY, lambda i, c: (n1_copy(i).wait_recv(), c)[1], 0)
    norm2_out[...] = jnp.sum(n1[...], axis=0)
    n2[z] = norm2_out[...]

    def n2_copy(i):
        return pltpu.make_async_remote_copy(
            src_ref=norm2_out, dst_ref=n2.at[z], send_sem=n2_ssem.at[i], recv_sem=n2_rsem.at[i],
            device_id=at(z + i, y), device_id_type=MESH)

    lax.fori_loop(1, nz, lambda i, c: (n2_copy(i).start(), c)[1], 0)
    for i in range(1, NY):
        for copy in x_copies(i):
            copy.wait_recv()
    lax.fori_loop(1, nz, lambda i, c: (n2_copy(i).wait_recv(), c)[1], 0)
    norm = jnp.sqrt(jnp.sum(jnp.sum(n2[...], axis=0), axis=1, keepdims=True))
    clip = 1.0 / jnp.maximum(norm, 1.0)

    states = [jnp.concatenate([t_in[a, k] for k in range(NY)], axis=0) for a in range(3)]
    w_ref[z, :, columns(y)] = adam(clip, total_q[...], *states)[0].astype(jnp.bfloat16)

    reach = (hz, hz - 1)

    def az_copy(way, t, stride):
        sign = 1 - 2 * way
        piece = w_ref.at[(z - sign * t + nz) % nz, :, columns(y)]
        return pltpu.make_async_remote_copy(
            src_ref=piece, dst_ref=piece, send_sem=az_ssem.at[way, t + stride], recv_sem=az_rsem.at[way, t + stride],
            device_id=at(z + sign * stride, y), device_id_type=MESH)

    def az_arrived(way, t):
        sign = 1 - 2 * way
        piece = w_ref.at[(z - sign * t + nz) % nz, :, columns(y)]
        pltpu.make_async_remote_copy(
            src_ref=piece, dst_ref=piece, send_sem=az_ssem.at[way, t], recv_sem=az_rsem.at[way, t],
            device_id=at(z - sign, y), device_id_type=MESH).wait_recv()

    def ag_tile(j):
        t = (j + 1) // 2
        sign = 1 - 2 * (j % 2)
        return (z + nz + sign * t) % nz

    def ay_copy(way, j, forward):
        yy = y if forward else (y - 1 + 2 * way + NY) % NY
        piece = w_ref.at[ag_tile(j), :, columns(yy)]
        return pltpu.make_async_remote_copy(
            src_ref=piece, dst_ref=piece, send_sem=ay_ssem.at[way, j], recv_sem=ay_rsem.at[way, j],
            device_id=at(z, y + 1 - 2 * way), device_id_type=MESH)

    def ar_copy(way, j, forward):
        q = ((y - 1 + 2 * way + NY) if forward else (y + 2)) % NY
        piece = w_ref.at[ag_tile(j), :, pl.ds(pl.multiple_of(q * quarter + way * half, 128), half)]
        return pltpu.make_async_remote_copy(
            src_ref=piece, dst_ref=piece, send_sem=ar_ssem.at[way, j], recv_sem=ar_rsem.at[way, j],
            device_id=at(z, y + 1 - 2 * way), device_id_type=MESH)

    def y_out(j):
        for way in (0, 1):
            ay_copy(way, j, True).start()

    def y_relay(j):
        for way in (0, 1):
            ay_copy(way, j, False).wait_recv()
            ar_copy(way, j, True).start()

    for stride in range(1, AG_STRIDE + 1):
        for way in (0, 1):
            if stride <= reach[way]:
                az_copy(way, 0, stride).start()
    y_out(0)

    for k in range(NY):
        cols = pl.ds(k * quarter, quarter)
        got = adam(clip, s_in[k], master_ref[:, cols], first_ref[:, cols], second_ref[:, cols])
        for ref, value in zip((o_master, o_first, o_second, o_direction), got):
            ref[:, cols] = value

    for t in range(1, hz + 1):
        for way in (0, 1):
            if t <= reach[way]:
                az_arrived(way, t)
                if t + AG_STRIDE <= reach[way]:
                    az_copy(way, t, AG_STRIDE).start()
                y_out(2 * t - 1 + way)
        if t == 1:
            y_relay(0)
        else:
            y_relay(2 * t - 3)
            y_relay(2 * t - 2)
    y_relay(nz - 1)

    def finish(j, carry):
        for way in (0, 1):
            ar_copy(way, j, False).wait_recv()
            y_copy(way, j).wait_send()
            relay(way, j).wait_send()
            ay_copy(way, j, True).wait_send()
            ar_copy(way, j, True).wait_send()
        return carry

    lax.fori_loop(0, nz, finish, 0)
    for h in (0, 1):
        for way in (0, 1):
            lax.fori_loop(way, hz, lambda i, c: (z_copy(way, i, h).wait_send(), c)[1], 0)
    for way in (0, 1):
        for t in range(1, reach[way] + 1):
            az_copy(way, max(t - AG_STRIDE, 0), min(t, AG_STRIDE)).wait_send()
    lax.fori_loop(1, n_e * NY, lambda i, c: (n1_copy(i).wait_send(), c)[1], 0)
    lax.fori_loop(1, nz, lambda i, c: (n2_copy(i).wait_send(), c)[1], 0)
    for i in range(1, NY):
        for copy in x_copies(i):
            copy.wait_send()


def solution(mesh):
    n_e = mesh.shape["expert"]
    nz = mesh.shape["dp"] // NY

    def step(grads, master, first, second):
        rows, width = grads.shape[2:]
        quarter = width // NY
        half = quarter // 2
        own = master.shape[1:]
        g = grads.reshape(nz, 8, width)
        hz = nz // 2
        f32, bf16 = jnp.float32, jnp.bfloat16
        dma = pltpu.SemaphoreType.DMA
        vmem = pl.BlockSpec(memory_space=pltpu.VMEM)
        out = pl.pallas_call(
            functools.partial(kernel, n_e, nz, quarter),
            out_shape=[jax.ShapeDtypeStruct(own, f32)] * 4 + [jax.ShapeDtypeStruct((nz, 8, width), bf16)],
            in_specs=[pl.BlockSpec(memory_space=pl.ANY), vmem, vmem, vmem],
            out_specs=[vmem] * 5,
            scratch_shapes=[
                pltpu.VMEM((nz, 8, 3 * quarter), bf16),
                pltpu.VMEM((nz, 8, quarter), bf16),
                pltpu.VMEM((2, nz, 8, 3 * half), bf16),
                pltpu.VMEM((2, nz, 8, half), bf16),
                pltpu.VMEM((2, hz + 1, 2, 8, half), f32),
                pltpu.VMEM((2, hz, 2, 8, half), f32),
                pltpu.VMEM((8, quarter), f32),
                pltpu.VMEM((NY, 2, quarter), f32),
                pltpu.VMEM((NY, 2, quarter), f32),
                pltpu.VMEM((3, NY, 2, quarter), f32),
                pltpu.VMEM((1, 128), f32),
                pltpu.VMEM((n_e * NY, 1, 128), f32),
                pltpu.VMEM((1, 128), f32),
                pltpu.VMEM((nz, 1, 128), f32),
                dma((NY,)), dma((1,)),
                dma((2, nz)), dma((2, nz)), dma((2, nz)), dma((2, nz)),
                dma((2, hz, 2)), dma((2, hz + 1, 2)),
                dma((4, NY)), dma((4, NY)),
                dma((n_e * NY,)), dma((n_e * NY,)), dma((nz,)), dma((nz,)),
                dma((2, hz + 1)), dma((2, hz + 1)),
                dma((2, nz)), dma((2, nz)), dma((2, nz)), dma((2, nz)),
            ],
            compiler_params=pltpu.CompilerParams(collective_id=0, has_side_effects=True),
        )(g, master.reshape(own), first.reshape(own), second.reshape(own))
        o_master, o_first, o_second, o_direction, w = out
        f = lambda a: a.reshape((1,) + own)
        return f(o_master), f(o_first), f(o_second), f(o_direction), w.reshape(1, rows, width)

    rows_spec = P("expert", "dp", None)
    return jax.shard_map(
        step,
        mesh=mesh,
        in_specs=(P("expert", "dp", None, None), rows_spec, rows_spec, rows_spec),
        out_specs=(rows_spec, rows_spec, rows_spec, rows_spec, P("expert", None, None)),
        check_vma=False,
    )
```

```python
import functools

import jax
import jax.numpy as jnp
from jax import lax
from jax.experimental import pallas as pl
from jax.experimental.pallas import tpu as pltpu
from jax.sharding import PartitionSpec as P

STEP = 10
NY = 4
RS_STRIDE = 2
PARENT = {1: 0, 2: 0, 3: 1, 4: 2, 5: 3, 6: 4, 7: 5, 8: 6}
VMEM_LIMIT = 52 * 1024 * 1024
MESH = pl.DeviceIdType.MESH


def adam(clip, summed, master, first, second):
    clipped = clip * summed
    new_first = 0.9 * first + 0.1 * clipped
    new_second = 0.95 * second + 0.05 * (clipped * clipped)
    first_fix = 1.0 - 0.9**STEP
    second_fix = 1.0 - 0.95**STEP
    direction = new_first / first_fix / (jnp.sqrt(new_second / second_fix) + 1e-08)
    new_master = master - 0.001 * (direction + 0.1 * master)
    return new_master, new_first, new_second, direction


def kernel(
    n_e, nz, quarter,
    g_hbm, states_ref,
    outs, w_ref,
    g, yin, rin, zin, zout, total_q, s_out, s_in, t_in, norm_out, n1, norm2_out, n2,
    load_sem, send_sem, y_rsem, r_rsem, z_rsem, w_rsem, x_rsem, n1_rsem, n2_rsem,
):
    half = quarter // 2
    hz = nz // 2
    e = lax.axis_index("expert")
    d = lax.axis_index("dp")
    z = d // NY
    y = d % NY

    def at(zz, yy):
        return (e, ((zz + nz) % nz) * NY + (yy + NY) % NY)

    def columns(q):
        return pl.ds(pl.multiple_of(q * quarter, 128), quarter)

    for i in range(NY):
        pltpu.make_async_copy(
            g_hbm.at[:, :, columns((y + 1 + i) % NY)], g.at[:, :, pl.ds(i * quarter, quarter)], load_sem.at[0]).start()
    master_ref, first_ref, second_ref = (states_ref.at[a] for a in range(3))

    barrier = pltpu.get_barrier_semaphore()
    for dz in [sign * hop for hop in range(1, RS_STRIDE + 1) for sign in (1, -1)]:
        pl.semaphore_signal(barrier, inc=1, device_id=at(z + dz, y), device_id_type=MESH)

    peers = [((e + k) % n_e, (y + i) % NY) for k in range(n_e) for i in range(NY)][1:]
    for ee, yy in peers:
        pl.semaphore_signal(barrier, inc=1, device_id=(ee, z * NY + yy), device_id_type=MESH)
    pl.semaphore_wait(barrier, n_e * NY - 1 + 2 * RS_STRIDE)

    pltpu.make_async_copy(g, g, load_sem.at[0]).wait()

    def tile(j):
        i = (j + 1) // 2
        sign = 2 * (j % 2) - 1
        return (z + 2 * nz + sign * (hz - i)) % nz

    def y_copy(way, j):
        src = g.at[tile(j), :, pl.ds(way * 3 * half, 3 * half)]
        return pltpu.make_async_remote_copy(
            src_ref=src, dst_ref=yin.at[way, j], send_sem=send_sem.at[0], recv_sem=y_rsem.at[j],
            device_id=at(z, y + 1 - 2 * way), device_id_type=MESH)

    def relay(way, j):
        src = yin.at[way, j, :, pl.ds(2 * half if way == 0 else 0, half)]
        return pltpu.make_async_remote_copy(
            src_ref=src, dst_ref=rin.at[way, j], send_sem=send_sem.at[1], recv_sem=r_rsem.at[way, j],
            device_id=at(z, y + 1 - 2 * way), device_id_type=MESH)

    def z_copy(way, i, h, hop=RS_STRIDE):
        return pltpu.make_async_remote_copy(
            src_ref=zout.at[way, i, h], dst_ref=zin.at[way, i, h],
            send_sem=send_sem.at[2 + 7 * way], recv_sem=z_rsem.at[way, i, h],
            device_id=at(z + (1 - 2 * way) * hop, y), device_id_type=MESH)

    def arrive(j):
        pltpu.make_async_copy(yin.at[:, j], yin.at[:, j], y_rsem.at[j]).wait()
        for way in (0, 1):
            relay(way, j).start()

    def y_start(j):
        for way in (0, 1):
            y_copy(way, j).start()

    def y_sum(j, h):
        cols = pl.ds(h * half, half)
        own = g[tile(j), :, pl.ds(3 * quarter + h * half, half)].astype(jnp.float32)
        left = yin[0, j, :, cols].astype(jnp.float32)
        right = yin[1, j, :, pl.ds(half + h * half, half)].astype(jnp.float32)
        far = rin[h, j].astype(jnp.float32)
        return (own + left) + (right + far)

    def z_step(i, ways, begins, hop=RS_STRIDE):
        for h in (0, 1):
            for way in ways:
                j = 0 if isinstance(i, int) and i == 0 else 2 * i - 1 + way
                relay(h, j).wait_recv()
                value = y_sum(j, h)
                if not begins[way]:
                    z_copy(way, i - RS_STRIDE, h).wait_recv()
                    value = value + zin[way, i - RS_STRIDE, h]
                zout[way, i, h] = value
                z_copy(way, i, h, hop).start()

    def step(i):
        for j in (2 * i + 1, 2 * i + 2):
            if j < nz:
                arrive(j)
        for j in (2 * i + 5, 2 * i + 6):
            if j < nz:
                y_start(j)
        z_step(i, (0, 1) if i else (0,), tuple(i - RS_STRIDE < way for way in (0, 1)), min(RS_STRIDE, hz - i))

    for j in (0, 1, 2):
        y_start(j)

    arrive(0)
    for j in (3, 4):
        if j < nz:
            y_start(j)

    for i in range(min(3, hz - 1)):
        step(i)

    def middle(i, carry):
        arrive(2 * i + 1)
        arrive(2 * i + 2)
        pl.when(2 * i + 5 < nz)(lambda: y_start(2 * i + 5))
        pl.when(2 * i + 6 < nz)(lambda: y_start(2 * i + 6))
        z_step(i, (0, 1), (False, False))
        return carry

    lax.fori_loop(3, hz - 1, middle, 0)
    step(hz - 1)

    squares = jnp.zeros((8, half), jnp.float32)
    for h in (0, 1):
        relay(h, nz - 1).wait_recv()
        value = y_sum(nz - 1, h)
        for way in (0, 1):
            for i in range(max(hz - RS_STRIDE, way), hz):
                z_copy(way, i, h).wait_recv()
                value = value + zin[way, i, h]
        total_q[:, pl.ds(h * half, half)] = value
        squares = squares + value * value

    norm_out[...] = jnp.sum(jnp.sum(squares.reshape(8, half // 128, 128), axis=1), axis=0, keepdims=True)
    mine = e * NY + y
    n1[mine] = norm_out[...]

    def rows_of(ref, n):
        return ref.at[pl.ds(0, n)]

    for ee, yy in peers:
        pltpu.make_async_remote_copy(
            src_ref=norm_out, dst_ref=n1.at[mine], send_sem=send_sem.at[3], recv_sem=n1_rsem.at[0],
            device_id=(ee, z * NY + yy), device_id_type=MESH).start()

    for k in range(NY):
        s_out[k] = total_q[pl.ds(2 * k, 2), :]

    def x_copies(i):
        yy = (y + i) % NY
        copies = [pltpu.make_async_remote_copy(
            src_ref=s_out.at[yy], dst_ref=s_in.at[y], send_sem=send_sem.at[5], recv_sem=x_rsem.at[0],
            device_id=at(z, yy), device_id_type=MESH)]
        for a, ref in enumerate((master_ref, first_ref, second_ref)):
            copies.append(pltpu.make_async_remote_copy(
                src_ref=ref.at[:, columns(yy)], dst_ref=t_in.at[a, y],
                send_sem=send_sem.at[5], recv_sem=x_rsem.at[0],
                device_id=at(z, yy), device_id_type=MESH))
        return copies

    for i in range(1, NY):
        for copy in x_copies(i):
            copy.start()
    s_in[y] = s_out[y]
    for a, ref in enumerate((master_ref, first_ref, second_ref)):
        t_in[a, y] = ref[:, columns(y)]

    n1_rest = rows_of(n1, n_e * NY - 1)
    pltpu.make_async_copy(n1_rest, n1_rest, n1_rsem.at[0]).wait()

    norm2_out[...] = jnp.sum(n1[...], axis=0)
    n2[z] = norm2_out[...]

    for i in range(1, nz):
        pltpu.make_async_remote_copy(
            src_ref=norm2_out, dst_ref=n2.at[z], send_sem=send_sem.at[4], recv_sem=n2_rsem.at[0],
            device_id=at(z + i, y), device_id_type=MESH).start()

    pltpu.make_async_copy(t_in, t_in, x_rsem.at[0]).wait()

    n2_rest = rows_of(n2, nz - 1)
    pltpu.make_async_copy(n2_rest, n2_rest, n2_rsem.at[0]).wait()
    norm = jnp.sqrt(jnp.sum(jnp.sum(n2[...], axis=0), axis=1, keepdims=True))
    clip = 1.0 / jnp.maximum(norm, 1.0)

    states = [jnp.concatenate([t_in[a, k] for k in range(NY)], axis=0) for a in range(3)]
    w_ref[z, :, columns(y)] = adam(clip, total_q[...], *states)[0].astype(jnp.bfloat16)

    reach = (hz, hz - 1)

    def parent(way, t):
        return PARENT[t] if PARENT[t] <= reach[way] else 0

    def az_copy(way, t, hop):
        sign = 1 - 2 * way
        piece = w_ref.at[(z - sign * (t - hop) + nz) % nz, :, columns(y)]
        return pltpu.make_async_remote_copy(
            src_ref=piece, dst_ref=piece, send_sem=send_sem.at[6], recv_sem=z_rsem.at[way, t - 1, 0],
            device_id=at(z + sign * hop, y), device_id_type=MESH)

    def az_pass(way, t):
        for child in PARENT:
            if child <= reach[way] and parent(way, child) == t:
                az_copy(way, child, child - t).start()

    def ag_tile(j):
        t = (j + 1) // 2
        sign = 1 - 2 * (j % 2)
        return (z + nz + sign * t) % nz

    def ay_copy(way, j, forward):
        yy = y if forward else (y - 1 + 2 * way + NY) % NY
        piece = w_ref.at[ag_tile(j), :, columns(yy)]
        return pltpu.make_async_remote_copy(
            src_ref=piece, dst_ref=piece, send_sem=send_sem.at[7], recv_sem=y_rsem.at[j],
            device_id=at(z, y + 1 - 2 * way), device_id_type=MESH)

    def ar_copy(way, j, forward):
        q = ((y - 1 + 2 * way + NY) if forward else (y + 2)) % NY
        piece = w_ref.at[ag_tile(j), :, pl.ds(pl.multiple_of(q * quarter + way * half, 128), half)]
        return pltpu.make_async_remote_copy(
            src_ref=piece, dst_ref=piece, send_sem=send_sem.at[8], recv_sem=w_rsem.at[0],
            device_id=at(z, y + 1 - 2 * way), device_id_type=MESH)

    def y_out(j):
        for way in (0, 1):
            ay_copy(way, j, True).start()

    two = w_ref.at[pl.ds(0, 2), :, pl.ds(0, quarter)]

    def y_relay(j):
        pltpu.make_async_copy(two, two, y_rsem.at[j]).wait()
        for way in (0, 1):
            ar_copy(way, j, True).start()

    for way in (0, 1):
        az_pass(way, 0)
    y_out(0)

    for k in range(NY):
        cols = pl.ds(k * quarter, quarter)
        got = adam(clip, s_in[k], master_ref[:, cols], first_ref[:, cols], second_ref[:, cols])
        for a, value in enumerate(got):
            outs[a, :, cols] = value

    before = [0]
    for t in [t for t in PARENT if t <= hz]:
        here = []
        for way in (0, 1):
            if t <= reach[way]:
                az_copy(way, t, t - parent(way, t)).wait_recv()
                az_pass(way, t)
                here.append(2 * t - 1 + way)
                y_out(here[-1])
        for j in before:
            y_relay(j)
        before = here
    for j in before:
        y_relay(j)

    relayed = w_ref.at[:, :, pl.ds(0, quarter)]
    pltpu.make_async_copy(relayed, relayed, w_rsem.at[0]).wait()
    sent = (
        (0, yin), (1, rin), (2, zout.at[0]), (9, zout.at[1, pl.ds(1, hz - 1)]), (3, n1_rest), (4, n2_rest), (5, t_in),
        (6, w_ref.at[pl.ds(0, nz - 1), :, pl.ds(0, quarter)]), (7, w_ref.at[:, :, pl.ds(0, 2 * quarter)]), (8, relayed),
    )
    for i, ref in sent:
        pltpu.make_async_copy(ref, ref, send_sem.at[i]).wait()


def emit(outs, w, *refs):
    sem = refs[5]
    copies = [pltpu.make_async_copy(w, refs[4], sem.at[4])]
    copies += [pltpu.make_async_copy(outs.at[a], refs[a], sem.at[a]) for a in range(4)]
    for copy in copies:
        copy.start()
    for copy in copies:
        copy.wait()


def solution(mesh):
    n_e = mesh.shape["expert"]
    nz = mesh.shape["dp"] // NY

    def step(grads, master, first, second):
        rows, width = grads.shape[2:]
        quarter = width // NY
        half = quarter // 2
        own = master.shape[1:]
        g = grads.reshape(nz, 8, width)
        hz = nz // 2
        f32, bf16 = jnp.float32, jnp.bfloat16
        dma = pltpu.SemaphoreType.DMA
        hbm = pl.BlockSpec(memory_space=pltpu.HBM)
        vmem = pl.BlockSpec(memory_space=pltpu.VMEM)
        out = pl.pallas_call(
            functools.partial(kernel, n_e, nz, quarter),
            out_shape=[jax.ShapeDtypeStruct((4,) + own, f32), jax.ShapeDtypeStruct((nz, 8, width), bf16)],
            in_specs=[hbm, vmem],
            out_specs=[vmem] * 2,
            scratch_shapes=[
                pltpu.VMEM((nz, 8, width), bf16),
                pltpu.VMEM((2, nz, 8, 3 * half), bf16),
                pltpu.VMEM((2, nz, 8, half), bf16),
                pltpu.VMEM((2, hz, 2, 8, half), f32),
                pltpu.VMEM((2, hz, 2, 8, half), f32),
                pltpu.VMEM((8, quarter), f32),
                pltpu.VMEM((NY, 2, quarter), f32),
                pltpu.VMEM((NY, 2, quarter), f32),
                pltpu.VMEM((3, NY, 2, quarter), f32),
                pltpu.VMEM((1, 128), f32),
                pltpu.VMEM((n_e * NY, 1, 128), f32),
                pltpu.VMEM((1, 128), f32),
                pltpu.VMEM((nz, 1, 128), f32),
                dma((1,)), dma((10,)), dma((nz,)), dma((2, nz)), dma((2, hz, 2)), dma((1,)), dma((1,)), dma((1,)), dma((1,)),
            ],
            compiler_params=pltpu.CompilerParams(collective_id=0, has_side_effects=True, vmem_limit_bytes=VMEM_LIMIT),
        )(g, jnp.concatenate([master, first, second], axis=0))
        o_master, o_first, o_second, o_direction, w = pl.pallas_call(
            emit,
            out_shape=[jax.ShapeDtypeStruct(own, f32)] * 4 + [jax.ShapeDtypeStruct((nz, 8, width), bf16)],
            in_specs=[vmem] * 2,
            out_specs=[hbm] * 5,
            scratch_shapes=[dma((5,))],
            compiler_params=pltpu.CompilerParams(vmem_limit_bytes=VMEM_LIMIT),
        )(*out)
        f = lambda a: a.reshape((1,) + own)
        return f(o_master), f(o_first), f(o_second), f(o_direction), w.reshape(1, rows, width)

    rows_spec = P("expert", "dp", None)
    return jax.shard_map(
        step,
        mesh=mesh,
        in_specs=(P("expert", "dp", None, None), rows_spec, rows_spec, rows_spec),
        out_specs=(rows_spec, rows_spec, rows_spec, rows_spec, P("expert", None, None)),
        check_vma=False,
    )
```

```python
import functools

import jax
import jax.numpy as jnp
from jax import lax
from jax.experimental import pallas as pl
from jax.experimental.pallas import tpu as pltpu
from jax.sharding import PartitionSpec as P

STEP = 10
NY = 4
LEAD = 2
RS_ORDER = (8, 7, 5, 6, 4, 2, 3, 1)
RS_PARENT = {8: 6, 7: 6, 6: 3, 5: 3, 4: 3, 3: 0, 2: 0, 1: 0}
RS_REACH = max(t - p for t, p in RS_PARENT.items())
AG_LAG = 2
DIAGONAL = (7, 8)
PARENT = {2: 1, 3: 1, 4: 1, 5: 4, 6: 4, 7: 6, 8: 6}
VMEM_LIMIT = 52 * 1024 * 1024
MESH = pl.DeviceIdType.MESH


def adam(clip, summed, master, first, second):
    clipped = clip * summed
    new_first = 0.9 * first + 0.1 * clipped
    new_second = 0.95 * second + 0.05 * (clipped * clipped)
    first_fix = 1.0 - 0.9**STEP
    second_fix = 1.0 - 0.95**STEP
    direction = new_first / first_fix / (jnp.sqrt(new_second / second_fix) + 1e-08)
    new_master = master - 0.001 * (direction + 0.1 * master)
    return new_master, new_first, new_second, direction


def kernel(
    n_e, nz, quarter,
    g_hbm, states_ref,
    outs, w_ref,
    g, ain, bin_, rin, zin, zout, total_q, near, s_out, s_in, t_in, norm_out, n1, norm2_out, n2,
    load_sem, send_sem, a_rsem, b_rsem, r_rsem, y_rsem, z_rsem, w_rsem, x_rsem, t_rsem, near_rsem, q_rsem, n1_rsem, n2_rsem,
):
    half = quarter // 2
    hz = nz // 2
    e = lax.axis_index("expert")
    d = lax.axis_index("dp")
    z = d // NY
    y = d % NY

    def at(zz, yy):
        return (e, ((zz + nz) % nz) * NY + (yy + NY) % NY)

    def columns(q):
        return pl.ds(pl.multiple_of(q * quarter, 128), quarter)

    for i in range(NY):
        pltpu.make_async_copy(
            g_hbm.at[:, :, columns((y + 1 + i) % NY)], g.at[:, :, pl.ds(i * quarter, quarter)], load_sem.at[0]).start()

    barrier = pltpu.get_barrier_semaphore()
    for dz in [sign * hop for hop in range(1, RS_REACH + 1) for sign in (1, -1)]:
        pl.semaphore_signal(barrier, inc=1, device_id=at(z + dz, y), device_id_type=MESH)

    peers = [((e + k) % n_e, (y + i) % NY) for k in range(n_e) for i in range(NY)][1:]
    for ee, yy in peers:
        pl.semaphore_signal(barrier, inc=1, device_id=(ee, z * NY + yy), device_id_type=MESH)
    pl.semaphore_wait(barrier, n_e * NY - 1 + 2 * RS_REACH)

    pltpu.make_async_copy(g, g, load_sem.at[0]).wait()

    order = [t for t in RS_ORDER if t <= hz]
    reach = (hz, hz - 1)

    def children(way, t):
        return [order.index(c) for c in order if RS_PARENT[c] == t and c <= reach[way]]

    def tile(j):
        t = (order + [0])[(j + 1) // 2]
        return (z + nz + t * (2 * (j % 2) - 1 if j else 1)) % nz

    def tiles(i):
        return (0, 1) if i == 0 else (2 * i - 1, 1 if i == hz else 2)

    def y_send(way, j, i, src, dst, send, recv):
        pltpu.make_async_remote_copy(
            src_ref=src, dst_ref=dst, send_sem=send_sem.at[send], recv_sem=recv.at[i],
            device_id=at(z, y + 1 - 2 * way), device_id_type=MESH).start()

    def ahead(i):
        first, n = tiles(i)
        for k in range(n):
            for way in (0, 1):
                src = g.at[tile(first + k), :, pl.ds(quarter + way * half, half)]
                y_send(way, first + k, i, src, ain.at[way, first + k], 0, a_rsem)

    def direct(i):
        first, n = tiles(i)
        for k in range(n):
            for way in (0, 1):
                src = g.at[tile(first + k), :, pl.ds(2 * way * quarter, quarter)]
                y_send(way, first + k, i, src, bin_.at[way, first + k], 1, b_rsem)

    def arrived(i, ref, sem):
        first, n = tiles(i)
        piece = ref.at[:, pl.ds(first, n)]
        pltpu.make_async_copy(piece, piece, sem.at[i]).wait()

    def relay(i):
        arrived(i, ain, a_rsem)
        first, n = tiles(i)
        for k in range(n):
            for way in (0, 1):
                y_send(way, first + k, i, ain.at[way, first + k], rin.at[way, first + k], 8, r_rsem)

    def z_copy(way, i, h):
        hop = order[i] - RS_PARENT[order[i]]
        return pltpu.make_async_remote_copy(
            src_ref=zout.at[way, i, h], dst_ref=zin.at[way, i, h],
            send_sem=send_sem.at[2 + 7 * way], recv_sem=z_rsem.at[way, i, h],
            device_id=at(z + (1 - 2 * way) * hop, y), device_id_type=MESH)

    def add_arrived(value, way, t, h):
        for i in children(way, t):
            z_copy(way, i, h).wait_recv()
            value = value + zin[way, i, h]
        return value

    def y_sum(j, h):
        cols = pl.ds(h * half, half)
        own = g[tile(j), :, pl.ds(3 * quarter + h * half, half)].astype(jnp.float32)
        left = bin_[0, j, :, cols].astype(jnp.float32)
        right = bin_[1, j, :, cols].astype(jnp.float32)
        far = rin[h, j].astype(jnp.float32)
        return (own + left) + (right + far)

    def step(i):
        if i + LEAD <= hz:
            relay(i + LEAD)
        if i + 2 + LEAD <= hz:
            ahead(i + 2 + LEAD)
        if i + 2 <= hz:
            direct(i + 2)
        arrived(i, bin_, b_rsem)
        arrived(i, rin, r_rsem)
        for h in (0, 1):
            for way in (0, 1) if i else (0,):
                zout[way, i, h] = add_arrived(y_sum(tiles(i)[0] + way, h), way, order[i], h)
                z_copy(way, i, h).start()

    for way in (0, 1):
        pltpu.make_async_remote_copy(
            src_ref=states_ref, dst_ref=near.at[way], send_sem=send_sem.at[11], recv_sem=near_rsem.at[0],
            device_id=at(z + 1 - 2 * way, y), device_id_type=MESH).start()

    def give_states():
        pltpu.make_async_copy(near, near, near_rsem.at[0]).wait()
        for i in range(1, NY):
            yy = (y + i) % NY
            for src, dst, send in (
                (states_ref.at[:, :, columns(yy)], t_in.at[0, :, y], 12),
                (near.at[:, :, :, columns(yy)], t_in.at[pl.ds(1, 2), :, y], 13),
            ):
                pltpu.make_async_remote_copy(
                    src_ref=src, dst_ref=dst, send_sem=send_sem.at[send], recv_sem=t_rsem.at[0],
                    device_id=at(z, yy), device_id_type=MESH).start()
        for a in range(3):
            t_in[0, a, y] = states_ref[a, :, columns(y)]
            for way in (0, 1):
                t_in[1 + way, a, y] = near[way, a, :, columns(y)]

    for i in range(LEAD + 1):
        if i <= hz:
            ahead(i)
    direct(0)
    if LEAD + 1 <= hz:
        ahead(LEAD + 1)
    direct(1)

    for i in range(LEAD):
        if i <= hz:
            relay(i)

    for i in range(hz):
        step(i)
    give_states()

    squares = jnp.zeros((8, half), jnp.float32)
    arrived(hz, bin_, b_rsem)
    arrived(hz, rin, r_rsem)
    for h in (0, 1):
        value = y_sum(nz - 1, h)
        for way in (0, 1):
            value = add_arrived(value, way, 0, h)
        total_q[0, :, pl.ds(h * half, half)] = value
        squares = squares + value * value

    norm_out[...] = jnp.sum(jnp.sum(squares.reshape(8, half // 128, 128), axis=1), axis=0, keepdims=True)
    mine = e * NY + y
    n1[mine] = norm_out[...]

    def rows_of(ref, n):
        return ref.at[pl.ds(0, n)]

    for ee, yy in peers:
        pltpu.make_async_remote_copy(
            src_ref=norm_out, dst_ref=n1.at[mine], send_sem=send_sem.at[3], recv_sem=n1_rsem.at[0],
            device_id=(ee, z * NY + yy), device_id_type=MESH).start()

    for way in (0, 1):
        pltpu.make_async_remote_copy(
            src_ref=total_q.at[0], dst_ref=total_q.at[1 + way], send_sem=send_sem.at[14], recv_sem=q_rsem.at[0],
            device_id=at(z + 1 - 2 * way, y), device_id_type=MESH).start()
    for k in range(NY):
        s_out[k] = total_q[0, pl.ds(2 * k, 2), :]
    for i in range(1, NY):
        yy = (y + i) % NY
        pltpu.make_async_remote_copy(
            src_ref=s_out.at[yy], dst_ref=s_in.at[y], send_sem=send_sem.at[5], recv_sem=x_rsem.at[0],
            device_id=at(z, yy), device_id_type=MESH).start()
    s_in[y] = s_out[y]

    n1_rest = rows_of(n1, n_e * NY - 1)
    pltpu.make_async_copy(n1_rest, n1_rest, n1_rsem.at[0]).wait()

    norm2_out[...] = jnp.sum(n1[...], axis=0)
    n2[z] = norm2_out[...]

    for i in range(1, nz):
        pltpu.make_async_remote_copy(
            src_ref=norm2_out, dst_ref=n2.at[z], send_sem=send_sem.at[4], recv_sem=n2_rsem.at[0],
            device_id=at(z + i, y), device_id_type=MESH).start()

    s_rest, t_rest, q_rest = s_in.at[pl.ds(0, NY - 1)], t_in.at[:, :, pl.ds(0, NY - 1)], total_q.at[pl.ds(1, 2)]
    for ref, sem in ((s_rest, x_rsem), (t_rest, t_rsem), (q_rest, q_rsem)):
        pltpu.make_async_copy(ref, ref, sem.at[0]).wait()

    n2_rest = rows_of(n2, nz - 1)
    pltpu.make_async_copy(n2_rest, n2_rest, n2_rsem.at[0]).wait()
    norm = jnp.sqrt(jnp.sum(jnp.sum(n2[...], axis=0), axis=1, keepdims=True))
    clip = 1.0 / jnp.maximum(norm, 1.0)

    def update(c, carry):
        states = [jnp.concatenate([t_in[c, a, k] for k in range(NY)], axis=0) for a in range(3)]
        new = adam(clip, total_q[c], *states)[0]
        w_ref[(z + nz + c // 2 - c % 2) % nz, :, columns(y)] = new.astype(jnp.bfloat16)
        return carry

    lax.fori_loop(0, 3, update, 0)

    def az_copy(way, t, hop):
        sign = 1 - 2 * way
        piece = w_ref.at[(z - sign * (t - hop) + nz) % nz, :, columns(y)]
        return pltpu.make_async_remote_copy(
            src_ref=piece, dst_ref=piece, send_sem=send_sem.at[6], recv_sem=z_rsem.at[way, t - 1, 0],
            device_id=at(z + sign * hop, y), device_id_type=MESH)

    def diagonal(way, t, hop):
        sign = 1 - 2 * way
        piece = w_ref.at[(z - sign * (t - hop) + nz) % nz, :, columns(y)]
        j = 2 * t - 1 + way
        for i in (1, 3, 2):
            pltpu.make_async_remote_copy(
                src_ref=piece, dst_ref=piece, send_sem=send_sem.at[7 if i != 2 else 10],
                recv_sem=y_rsem.at[j] if i != 2 else w_rsem.at[0],
                device_id=at(z + sign * hop, y + i), device_id_type=MESH).start()

    def az_pass(way, t):
        for child in PARENT:
            if child <= reach[way] and PARENT[child] == t:
                az_copy(way, child, child - t).start()
                if child in DIAGONAL:
                    diagonal(way, child, child - t)

    def ag_tile(j):
        t = (j + 1) // 2
        sign = 1 - 2 * (j % 2)
        return (z + nz + sign * t) % nz

    def ay_copy(way, j, forward):
        yy = y if forward else (y - 1 + 2 * way + NY) % NY
        piece = w_ref.at[ag_tile(j), :, columns(yy)]
        return pltpu.make_async_remote_copy(
            src_ref=piece, dst_ref=piece, send_sem=send_sem.at[7], recv_sem=y_rsem.at[j],
            device_id=at(z, y + 1 - 2 * way), device_id_type=MESH)

    def ar_copy(way, j, forward):
        q = ((y - 1 + 2 * way + NY) if forward else (y + 2)) % NY
        piece = w_ref.at[ag_tile(j), :, pl.ds(pl.multiple_of(q * quarter + way * half, 128), half)]
        return pltpu.make_async_remote_copy(
            src_ref=piece, dst_ref=piece, send_sem=send_sem.at[10], recv_sem=w_rsem.at[0],
            device_id=at(z, y + 1 - 2 * way), device_id_type=MESH)

    def y_out(j):
        for way in (0, 1):
            ay_copy(way, j, True).start()

    two = w_ref.at[pl.ds(0, 2), :, pl.ds(0, quarter)]

    def y_relay(j):
        pltpu.make_async_copy(two, two, y_rsem.at[j]).wait()
        for way in (0, 1):
            ar_copy(way, j, True).start()

    for way in (0, 1):
        az_pass(way, 1)
    for j in range(3):
        y_out(j)

    for k in range(NY):
        cols = pl.ds(k * quarter, quarter)
        got = adam(clip, s_in[k], *[states_ref[a, :, cols] for a in range(3)])
        for a, value in enumerate(got):
            outs[a, :, cols] = value

    waiting, last = [[0, 1, 2]], []
    for t in [t for t in PARENT if t <= hz]:
        here = []
        for way in (0, 1):
            if t <= reach[way]:
                az_copy(way, t, t - PARENT[t]).wait_recv()
                az_pass(way, t)
                here.append(2 * t - 1 + way)
                if t in DIAGONAL:
                    last.append(here.pop())
                else:
                    y_out(here[-1])
        waiting.append(here)
        if len(waiting) > AG_LAG:
            for j in waiting.pop(0):
                y_relay(j)
    for j in sum(waiting, []):
        y_relay(j)
    for j in last:
        pltpu.make_async_copy(two, two, y_rsem.at[j]).wait()

    relayed = w_ref.at[:, :, pl.ds(0, quarter)]
    pltpu.make_async_copy(relayed, relayed, w_rsem.at[0]).wait()
    sent = (
        (0, ain), (1, bin_), (8, rin), (2, zout.at[0]), (9, zout.at[1, pl.ds(1, hz - 1)]), (3, n1_rest), (4, n2_rest), (5, s_rest), (11, near), (12, t_in.at[0, :, pl.ds(0, NY - 1)]),
        (13, t_in.at[pl.ds(1, 2), :, pl.ds(0, NY - 1)]), (14, q_rest),
        (6, w_ref.at[pl.ds(0, nz - 3), :, pl.ds(0, quarter)]), (7, w_ref.at[:, :, pl.ds(0, 2 * quarter)]), (10, relayed),
    )
    for i, ref in sent:
        pltpu.make_async_copy(ref, ref, send_sem.at[i]).wait()


def emit(outs, w, *refs):
    sem = refs[5]
    copies = [pltpu.make_async_copy(w, refs[4], sem.at[4])]
    copies += [pltpu.make_async_copy(outs.at[a], refs[a], sem.at[a]) for a in range(4)]
    for copy in copies:
        copy.start()
    for copy in copies:
        copy.wait()


def solution(mesh):
    n_e = mesh.shape["expert"]
    nz = mesh.shape["dp"] // NY

    def step(grads, master, first, second):
        rows, width = grads.shape[2:]
        quarter = width // NY
        half = quarter // 2
        own = master.shape[1:]
        g = grads.reshape(nz, 8, width)
        hz = nz // 2
        f32, bf16 = jnp.float32, jnp.bfloat16
        dma = pltpu.SemaphoreType.DMA
        hbm = pl.BlockSpec(memory_space=pltpu.HBM)
        vmem = pl.BlockSpec(memory_space=pltpu.VMEM)
        out = pl.pallas_call(
            functools.partial(kernel, n_e, nz, quarter),
            out_shape=[jax.ShapeDtypeStruct((4,) + own, f32), jax.ShapeDtypeStruct((nz, 8, width), bf16)],
            in_specs=[hbm, vmem],
            out_specs=[vmem] * 2,
            scratch_shapes=[
                pltpu.VMEM((nz, 8, width), bf16),
                pltpu.VMEM((2, nz, 8, half), bf16),
                pltpu.VMEM((2, nz, 8, quarter), bf16),
                pltpu.VMEM((2, nz, 8, half), bf16),
                pltpu.VMEM((2, hz, 2, 8, half), f32),
                pltpu.VMEM((2, hz, 2, 8, half), f32),
                pltpu.VMEM((3, 8, quarter), f32),
                pltpu.VMEM((2, 3) + own, f32),
                pltpu.VMEM((NY, 2, quarter), f32),
                pltpu.VMEM((NY, 2, quarter), f32),
                pltpu.VMEM((3, 3, NY, 2, quarter), f32),
                pltpu.VMEM((1, 128), f32),
                pltpu.VMEM((n_e * NY, 1, 128), f32),
                pltpu.VMEM((1, 128), f32),
                pltpu.VMEM((nz, 1, 128), f32),
                dma((1,)), dma((15,)), dma((hz + 1,)), dma((hz + 1,)), dma((hz + 1,)), dma((nz,)), dma((2, hz, 2)), *[dma((1,))] * 7,
            ],
            compiler_params=pltpu.CompilerParams(collective_id=0, has_side_effects=True, vmem_limit_bytes=VMEM_LIMIT),
        )(g, jnp.concatenate([master, first, second], axis=0))
        o_master, o_first, o_second, o_direction, w = pl.pallas_call(
            emit,
            out_shape=[jax.ShapeDtypeStruct(own, f32)] * 4 + [jax.ShapeDtypeStruct((nz, 8, width), bf16)],
            in_specs=[vmem] * 2,
            out_specs=[hbm] * 5,
            scratch_shapes=[dma((5,))],
            compiler_params=pltpu.CompilerParams(vmem_limit_bytes=VMEM_LIMIT),
        )(*out)
        f = lambda a: a.reshape((1,) + own)
        return f(o_master), f(o_first), f(o_second), f(o_direction), w.reshape(1, rows, width)

    rows_spec = P("expert", "dp", None)
    return jax.shard_map(
        step,
        mesh=mesh,
        in_specs=(P("expert", "dp", None, None), rows_spec, rows_spec, rows_spec),
        out_specs=(rows_spec, rows_spec, rows_spec, rows_spec, P("expert", None, None)),
        check_vma=False,
    )
```

```python
import functools

import jax
import jax.numpy as jnp
from jax import lax
from jax.experimental import pallas as pl
from jax.experimental.pallas import tpu as pltpu
from jax.sharding import PartitionSpec as P

STEP = 10
NY = 4
LEAD = 2
RS_ORDER = (8, 7, 5, 6, 4, 2, 3, 1)
RS_PARENT = {8: 6, 7: 6, 6: 3, 5: 3, 4: 3, 3: 0, 2: 0, 1: 0}
ROUNDS = 4
AG_LAG = 2
DIAGONAL = (7, 8)
PARENT = {2: 1, 3: 1, 4: 1, 5: 4, 6: 4, 7: 6, 8: 6}
VMEM_LIMIT = 52 * 1024 * 1024
MESH = pl.DeviceIdType.MESH


def adam(clip, summed, master, first, second):
    clipped = clip * summed
    new_first = 0.9 * first + 0.1 * clipped
    new_second = 0.95 * second + 0.05 * (clipped * clipped)
    first_fix = 1.0 - 0.9**STEP
    second_fix = 1.0 - 0.95**STEP
    direction = new_first / first_fix / (jnp.sqrt(new_second / second_fix) + 1e-08)
    new_master = master - 0.001 * (direction + 0.1 * master)
    return new_master, new_first, new_second, direction


def kernel(
    n_e, nz, quarter,
    g_hbm, states_ref,
    outs, w_ref,
    g, ain, bin_, rin, zin, zout, total_q, near, s_out, s_in, t_in, norm_out, n1, norm2_out, n2,
    load_sem, send_sem, a_rsem, b_rsem, r_rsem, y_rsem, z_rsem, w_rsem, x_rsem, t_rsem, near_rsem, q_rsem, n1_rsem, n2_rsem, met,
):
    half = quarter // 2
    hz = nz // 2
    e = lax.axis_index("expert")
    d = lax.axis_index("dp")
    z = d // NY
    y = d % NY

    def at(zz, yy):
        return (e, ((zz + nz) % nz) * NY + (yy + NY) % NY)

    def columns(q):
        return pl.ds(pl.multiple_of(q * quarter, 128), quarter)

    for i in range(NY):
        pltpu.make_async_copy(
            g_hbm.at[:, :, columns((y + 1 + i) % NY)], g.at[:, :, pl.ds(i * quarter, quarter)], load_sem.at[0]).start()

    def other(ee):
        return ((ee + n_e) % n_e, d)

    neighbours = [at(z + 1, y), at(z - 1, y), at(z, y + 1), at(z, y - 1), other(e + 1 - 2 * (e % 2))]
    if n_e > 2:
        neighbours += [other(e + 2), other(e - 2)]

    def greet(sem):
        for device in neighbours:
            pl.semaphore_signal(sem, inc=1, device_id=device, device_id_type=MESH)

    barrier = pltpu.get_barrier_semaphore()
    greet(barrier)
    pl.semaphore_wait(barrier, len(neighbours))

    def round_(r):
        pl.semaphore_wait(met.at[r], len(neighbours))
        if r + 1 < ROUNDS:
            greet(met.at[r + 1])

    greet(met.at[0])

    pltpu.make_async_copy(g, g, load_sem.at[0]).wait()

    order = [t for t in RS_ORDER if t <= hz]
    reach = (hz, hz - 1)

    def children(way, t):
        return [order.index(c) for c in order if RS_PARENT[c] == t and c <= reach[way]]

    def tile(j):
        t = (order + [0])[(j + 1) // 2]
        return (z + nz + t * (2 * (j % 2) - 1 if j else 1)) % nz

    def tiles(i):
        return (0, 1) if i == 0 else (2 * i - 1, 1 if i == hz else 2)

    def y_send(way, j, i, src, dst, send, recv):
        pltpu.make_async_remote_copy(
            src_ref=src, dst_ref=dst, send_sem=send_sem.at[send], recv_sem=recv.at[i],
            device_id=at(z, y + 1 - 2 * way), device_id_type=MESH).start()

    def ahead(i):
        first, n = tiles(i)
        for k in range(n):
            for way in (0, 1):
                src = g.at[tile(first + k), :, pl.ds(quarter + way * half, half)]
                y_send(way, first + k, i, src, ain.at[way, first + k], 0, a_rsem)

    def direct(i):
        first, n = tiles(i)
        for k in range(n):
            for way in (0, 1):
                src = g.at[tile(first + k), :, pl.ds(2 * way * quarter, quarter)]
                y_send(way, first + k, i, src, bin_.at[way, first + k], 1, b_rsem)

    def arrived(i, ref, sem):
        first, n = tiles(i)
        piece = ref.at[:, pl.ds(first, n)]
        pltpu.make_async_copy(piece, piece, sem.at[i]).wait()

    def relay(i):
        arrived(i, ain, a_rsem)
        first, n = tiles(i)
        for k in range(n):
            for way in (0, 1):
                y_send(way, first + k, i, ain.at[way, first + k], rin.at[way, first + k], 8, r_rsem)

    def z_copy(way, i, h):
        hop = order[i] - RS_PARENT[order[i]]
        return pltpu.make_async_remote_copy(
            src_ref=zout.at[way, i, h], dst_ref=zin.at[way, i, h],
            send_sem=send_sem.at[2 + 7 * way], recv_sem=z_rsem.at[way, i, h],
            device_id=at(z + (1 - 2 * way) * hop, y), device_id_type=MESH)

    def add_arrived(value, way, t, h):
        for i in children(way, t):
            z_copy(way, i, h).wait_recv()
            value = value + zin[way, i, h]
        return value

    def y_sum(j, h):
        cols = pl.ds(h * half, half)
        own = g[tile(j), :, pl.ds(3 * quarter + h * half, half)].astype(jnp.float32)
        left = bin_[0, j, :, cols].astype(jnp.float32)
        right = bin_[1, j, :, cols].astype(jnp.float32)
        far = rin[h, j].astype(jnp.float32)
        return (own + left) + (right + far)

    def step(i):
        if i < ROUNDS:
            round_(i)
        if i + LEAD <= hz:
            relay(i + LEAD)
        if i + 2 + LEAD <= hz:
            ahead(i + 2 + LEAD)
        if i + 2 <= hz:
            direct(i + 2)
        arrived(i, bin_, b_rsem)
        arrived(i, rin, r_rsem)
        for h in (0, 1):
            for way in (0, 1) if i else (0,):
                zout[way, i, h] = add_arrived(y_sum(tiles(i)[0] + way, h), way, order[i], h)
                z_copy(way, i, h).start()

    for way in (0, 1):
        pltpu.make_async_remote_copy(
            src_ref=states_ref, dst_ref=near.at[way], send_sem=send_sem.at[11], recv_sem=near_rsem.at[0],
            device_id=at(z + 1 - 2 * way, y), device_id_type=MESH).start()

    def give_states():
        pltpu.make_async_copy(near, near, near_rsem.at[0]).wait()
        for i in range(1, NY):
            yy = (y + i) % NY
            for src, dst, send in (
                (states_ref.at[:, :, columns(yy)], t_in.at[0, :, y], 12),
                (near.at[:, :, :, columns(yy)], t_in.at[pl.ds(1, 2), :, y], 13),
            ):
                pltpu.make_async_remote_copy(
                    src_ref=src, dst_ref=dst, send_sem=send_sem.at[send], recv_sem=t_rsem.at[0],
                    device_id=at(z, yy), device_id_type=MESH).start()
        for a in range(3):
            t_in[0, a, y] = states_ref[a, :, columns(y)]
            for way in (0, 1):
                t_in[1 + way, a, y] = near[way, a, :, columns(y)]

    for i in range(LEAD + 1):
        if i <= hz:
            ahead(i)
    direct(0)
    if LEAD + 1 <= hz:
        ahead(LEAD + 1)
    direct(1)

    for i in range(LEAD):
        if i <= hz:
            relay(i)

    for i in range(hz):
        step(i)
    give_states()

    squares = jnp.zeros((8, half), jnp.float32)
    arrived(hz, bin_, b_rsem)
    arrived(hz, rin, r_rsem)
    for h in (0, 1):
        value = y_sum(nz - 1, h)
        for way in (0, 1):
            value = add_arrived(value, way, 0, h)
        total_q[0, :, pl.ds(h * half, half)] = value
        squares = squares + value * value

    norm_out[...] = jnp.sum(jnp.sum(squares.reshape(8, half // 128, 128), axis=1), axis=0, keepdims=True)
    mine = e * NY + y
    n1[mine] = norm_out[...]

    def far_first(n):
        return sorted(range(n), key=lambda i: -min(i, n - i))

    def n1_send(k, i):
        ee = ((e // 2 + k) % (n_e // 2)) * 2 + 1
        pltpu.make_async_remote_copy(
            src_ref=norm_out, dst_ref=n1.at[mine], send_sem=send_sem.at[3], recv_sem=n1_rsem.at[0],
            device_id=(ee, z * NY + (y + i) % NY), device_id_type=MESH).start()

    for k in far_first(n_e // 2):
        for i in far_first(NY):
            if k or i:
                n1_send(k, i)
    pl.when(e % 2 == 0)(lambda: n1_send(0, 0))

    for way in (0, 1):
        pltpu.make_async_remote_copy(
            src_ref=total_q.at[0], dst_ref=total_q.at[1 + way], send_sem=send_sem.at[14], recv_sem=q_rsem.at[0],
            device_id=at(z + 1 - 2 * way, y), device_id_type=MESH).start()
    for k in range(NY):
        s_out[k] = total_q[0, pl.ds(2 * k, 2), :]
    for i in range(1, NY):
        yy = (y + i) % NY
        pltpu.make_async_remote_copy(
            src_ref=s_out.at[yy], dst_ref=s_in.at[y], send_sem=send_sem.at[5], recv_sem=x_rsem.at[0],
            device_id=at(z, yy), device_id_type=MESH).start()
    s_in[y] = s_out[y]

    def wait_rows(ref, n, sem):
        piece = ref.at[pl.ds(0, n)]
        pltpu.make_async_copy(piece, piece, sem).wait()

    def n2_send(i, core):
        pltpu.make_async_remote_copy(
            src_ref=norm2_out, dst_ref=n2.at[z], send_sem=send_sem.at[4], recv_sem=n2_rsem.at[0],
            device_id=(e - 1 + core, ((z + i) % nz) * NY + y), device_id_type=MESH).start()

    @pl.when(e % 2 == 1)
    def _():
        wait_rows(n1, n_e * NY - 1, n1_rsem.at[0])
        norm2_out[...] = jnp.sum(n1[...], axis=0)
        n2[z] = norm2_out[...]
        for i in far_first(nz):
            n2_send(i, 0)
            if i:
                n2_send(i, 1)

    s_rest, t_rest, q_rest = s_in.at[pl.ds(0, NY - 1)], t_in.at[:, :, pl.ds(0, NY - 1)], total_q.at[pl.ds(1, 2)]
    for ref, sem in ((s_rest, x_rsem), (t_rest, t_rsem), (q_rest, q_rsem)):
        pltpu.make_async_copy(ref, ref, sem.at[0]).wait()

    pl.when(e % 2 == 1)(lambda: wait_rows(n2, nz - 1, n2_rsem.at[0]))
    pl.when(e % 2 == 0)(lambda: wait_rows(n2, nz, n2_rsem.at[0]))
    norm = jnp.sqrt(jnp.sum(jnp.sum(n2[...], axis=0), axis=1, keepdims=True))
    clip = 1.0 / jnp.maximum(norm, 1.0)

    def update(c, carry):
        states = [jnp.concatenate([t_in[c, a, k] for k in range(NY)], axis=0) for a in range(3)]
        new = adam(clip, total_q[c], *states)[0]
        w_ref[(z + nz + c // 2 - c % 2) % nz, :, columns(y)] = new.astype(jnp.bfloat16)
        return carry

    lax.fori_loop(0, 3, update, 0)

    def az_copy(way, t, hop):
        sign = 1 - 2 * way
        piece = w_ref.at[(z - sign * (t - hop) + nz) % nz, :, columns(y)]
        return pltpu.make_async_remote_copy(
            src_ref=piece, dst_ref=piece, send_sem=send_sem.at[6], recv_sem=z_rsem.at[way, t - 1, 0],
            device_id=at(z + sign * hop, y), device_id_type=MESH)

    def diagonal(way, t, hop):
        sign = 1 - 2 * way
        piece = w_ref.at[(z - sign * (t - hop) + nz) % nz, :, columns(y)]
        j = 2 * t - 1 + way
        for i in (1, 3, 2):
            pltpu.make_async_remote_copy(
                src_ref=piece, dst_ref=piece, send_sem=send_sem.at[7 if i != 2 else 10],
                recv_sem=y_rsem.at[j] if i != 2 else w_rsem.at[0],
                device_id=at(z + sign * hop, y + i), device_id_type=MESH).start()

    def az_pass(way, t):
        far = [c for c in PARENT if PARENT[c] == t and c <= reach[way]]
        if t == 6:
            far = far[::-1]
        for child in far:
            if child in DIAGONAL:
                diagonal(way, child, child - t)
            az_copy(way, child, child - t).start()

    def ag_tile(j):
        t = (j + 1) // 2
        sign = 1 - 2 * (j % 2)
        return (z + nz + sign * t) % nz

    def ay_copy(way, j, forward):
        yy = y if forward else (y - 1 + 2 * way + NY) % NY
        piece = w_ref.at[ag_tile(j), :, columns(yy)]
        return pltpu.make_async_remote_copy(
            src_ref=piece, dst_ref=piece, send_sem=send_sem.at[7], recv_sem=y_rsem.at[j],
            device_id=at(z, y + 1 - 2 * way), device_id_type=MESH)

    def ar_copy(way, j, forward):
        q = ((y - 1 + 2 * way + NY) if forward else (y + 2)) % NY
        piece = w_ref.at[ag_tile(j), :, pl.ds(pl.multiple_of(q * quarter + way * half, 128), half)]
        return pltpu.make_async_remote_copy(
            src_ref=piece, dst_ref=piece, send_sem=send_sem.at[10], recv_sem=w_rsem.at[0],
            device_id=at(z, y + 1 - 2 * way), device_id_type=MESH)

    def y_out(j):
        for way in (0, 1):
            ay_copy(way, j, True).start()

    two = w_ref.at[pl.ds(0, 2), :, pl.ds(0, quarter)]

    def y_relay(j):
        pltpu.make_async_copy(two, two, y_rsem.at[j]).wait()
        for way in (0, 1):
            ar_copy(way, j, True).start()

    for way in (0, 1):
        az_pass(way, 1)
    for j in range(3):
        y_out(j)

    for k in range(NY):
        cols = pl.ds(k * quarter, quarter)
        got = adam(clip, s_in[k], *[states_ref[a, :, cols] for a in range(3)])
        for a, value in enumerate(got):
            outs[a, :, cols] = value

    waiting, leaves = [[0, 1, 2]], []
    for t in [t for t in PARENT if t <= hz]:
        here = []
        for way in (0, 1):
            if t > reach[way]:
                continue
            if t in DIAGONAL:
                leaves.append((way, t))
                continue
            az_copy(way, t, t - PARENT[t]).wait_recv()
            az_pass(way, t)
            here.append(2 * t - 1 + way)
            y_out(here[-1])
        if here:
            waiting.append(here)
            if len(waiting) > AG_LAG:
                for j in waiting.pop(0):
                    y_relay(j)
    for j in sum(waiting, []):
        y_relay(j)
    for way, t in leaves:
        az_copy(way, t, t - PARENT[t]).wait_recv()
        pltpu.make_async_copy(two, two, y_rsem.at[2 * t - 1 + way]).wait()

    relayed = w_ref.at[:, :, pl.ds(0, quarter)]
    pltpu.make_async_copy(relayed, relayed, w_rsem.at[0]).wait()
    sent = (
        (0, ain), (1, bin_), (8, rin), (2, zout.at[0]), (9, zout.at[1, pl.ds(1, hz - 1)]), (5, s_rest), (11, near), (12, t_in.at[0, :, pl.ds(0, NY - 1)]),
        (13, t_in.at[pl.ds(1, 2), :, pl.ds(0, NY - 1)]), (14, q_rest),
        (6, w_ref.at[pl.ds(0, nz - 3), :, pl.ds(0, quarter)]), (7, w_ref.at[:, :, pl.ds(0, 2 * quarter)]), (10, relayed),
    )
    wait_rows(n1, n_e * NY // 2 - 1, send_sem.at[3])
    pl.when(e % 2 == 0)(lambda: wait_rows(n1, 1, send_sem.at[3]))
    pl.when(e % 2 == 1)(lambda: wait_rows(n1, 2 * nz - 1, send_sem.at[4]))
    for i, ref in sent:
        pltpu.make_async_copy(ref, ref, send_sem.at[i]).wait()


def emit(outs, w, *refs):
    sem = refs[5]
    copies = [pltpu.make_async_copy(w, refs[4], sem.at[4])]
    copies += [pltpu.make_async_copy(outs.at[a], refs[a], sem.at[a]) for a in range(4)]
    for copy in copies:
        copy.start()
    for copy in copies:
        copy.wait()


def solution(mesh):
    n_e = mesh.shape["expert"]
    nz = mesh.shape["dp"] // NY

    def step(grads, master, first, second):
        rows, width = grads.shape[2:]
        quarter = width // NY
        half = quarter // 2
        own = master.shape[1:]
        g = grads.reshape(nz, 8, width)
        hz = nz // 2
        f32, bf16 = jnp.float32, jnp.bfloat16
        dma = pltpu.SemaphoreType.DMA
        hbm = pl.BlockSpec(memory_space=pltpu.HBM)
        vmem = pl.BlockSpec(memory_space=pltpu.VMEM)
        out = pl.pallas_call(
            functools.partial(kernel, n_e, nz, quarter),
            out_shape=[jax.ShapeDtypeStruct((4,) + own, f32), jax.ShapeDtypeStruct((nz, 8, width), bf16)],
            in_specs=[hbm, vmem],
            out_specs=[vmem] * 2,
            scratch_shapes=[
                pltpu.VMEM((nz, 8, width), bf16),
                pltpu.VMEM((2, nz, 8, half), bf16),
                pltpu.VMEM((2, nz, 8, quarter), bf16),
                pltpu.VMEM((2, nz, 8, half), bf16),
                pltpu.VMEM((2, hz, 2, 8, half), f32),
                pltpu.VMEM((2, hz, 2, 8, half), f32),
                pltpu.VMEM((3, 8, quarter), f32),
                pltpu.VMEM((2, 3) + own, f32),
                pltpu.VMEM((NY, 2, quarter), f32),
                pltpu.VMEM((NY, 2, quarter), f32),
                pltpu.VMEM((3, 3, NY, 2, quarter), f32),
                pltpu.VMEM((1, 128), f32),
                pltpu.VMEM((n_e * NY, 1, 128), f32),
                pltpu.VMEM((1, 128), f32),
                pltpu.VMEM((nz, 1, 128), f32),
                dma((1,)), dma((15,)), dma((hz + 1,)), dma((hz + 1,)), dma((hz + 1,)), dma((nz,)), dma((2, hz, 2)), *[dma((1,))] * 7, pltpu.SemaphoreType.REGULAR((ROUNDS,)),
            ],
            compiler_params=pltpu.CompilerParams(collective_id=0, has_side_effects=True, vmem_limit_bytes=VMEM_LIMIT),
        )(g, jnp.concatenate([master, first, second], axis=0))
        o_master, o_first, o_second, o_direction, w = pl.pallas_call(
            emit,
            out_shape=[jax.ShapeDtypeStruct(own, f32)] * 4 + [jax.ShapeDtypeStruct((nz, 8, width), bf16)],
            in_specs=[vmem] * 2,
            out_specs=[hbm] * 5,
            scratch_shapes=[dma((5,))],
            compiler_params=pltpu.CompilerParams(vmem_limit_bytes=VMEM_LIMIT),
        )(*out)
        f = lambda a: a.reshape((1,) + own)
        return f(o_master), f(o_first), f(o_second), f(o_direction), w.reshape(1, rows, width)

    rows_spec = P("expert", "dp", None)
    return jax.shard_map(
        step,
        mesh=mesh,
        in_specs=(P("expert", "dp", None, None), rows_spec, rows_spec, rows_spec),
        out_specs=(rows_spec, rows_spec, rows_spec, rows_spec, P("expert", None, None)),
        check_vma=False,
    )
```

```python
import functools

import jax
import jax.numpy as jnp
from jax import lax
from jax.experimental import pallas as pl
from jax.experimental.pallas import tpu as pltpu
from jax.sharding import PartitionSpec as P

STEP = 10
NY = 4
LEAD = 1
RS_ORDER = (8, 7, 5, 6, 4, 2, 3, 1)
RS_PARENT = {8: 6, 7: 6, 6: 3, 5: 3, 4: 3, 3: 0, 2: 0, 1: 0}
ROUNDS = 4
AG_LAG = 2
DIAGONAL = (7, 8)
PARENT = {2: 1, 3: 1, 4: 1, 5: 4, 6: 4, 7: 6, 8: 6}
VMEM_LIMIT = 52 * 1024 * 1024
MESH = pl.DeviceIdType.MESH


def adam(clip, summed, master, first, second):
    clipped = clip * summed
    new_first = 0.9 * first + 0.1 * clipped
    new_second = 0.95 * second + 0.05 * (clipped * clipped)
    first_fix = 1.0 - 0.9**STEP
    second_fix = 1.0 - 0.95**STEP
    direction = new_first / first_fix / (jnp.sqrt(new_second / second_fix) + 1e-08)
    new_master = master - 0.001 * (direction + 0.1 * master)
    return new_master, new_first, new_second, direction


def kernel(
    n_e, nz, quarter,
    g_hbm, states_ref,
    outs, w_ref,
    g, ain, bin_, rin, zin, zout, total_q, near, s_out, s_in, t_in, norm_out, n1, norm2_out, n2,
    load_sem, send_sem, a_rsem, b_rsem, r_rsem, y_rsem, z_rsem, w_rsem, x_rsem, t_rsem, near_rsem, q_rsem, n1_rsem, n2_rsem, met,
):
    half = quarter // 2
    hz = nz // 2
    e = lax.axis_index("expert")
    d = lax.axis_index("dp")
    z = d // NY
    y = d % NY

    def at(zz, yy):
        return (e, ((zz + nz) % nz) * NY + (yy + NY) % NY)

    def columns(q):
        return pl.ds(pl.multiple_of(q * quarter, 128), quarter)

    for i in range(NY):
        pltpu.make_async_copy(
            g_hbm.at[:, :, columns((y + 1 + i) % NY)], g.at[:, :, pl.ds(i * quarter, quarter)], load_sem.at[0]).start()

    def other(ee):
        return ((ee + n_e) % n_e, d)

    neighbours = [at(z + 1, y), at(z - 1, y), at(z, y + 1), at(z, y - 1), other(e + 1 - 2 * (e % 2))]
    if n_e > 2:
        neighbours += [other(e + 2), other(e - 2)]

    def greet(sem):
        for device in neighbours:
            pl.semaphore_signal(sem, inc=1, device_id=device, device_id_type=MESH)

    barrier = pltpu.get_barrier_semaphore()
    greet(barrier)
    pl.semaphore_wait(barrier, len(neighbours))

    def round_(r):
        pl.semaphore_wait(met.at[r], len(neighbours))
        if r + 1 < ROUNDS:
            greet(met.at[r + 1])

    greet(met.at[0])

    pltpu.make_async_copy(g, g, load_sem.at[0]).wait()

    order = [t for t in RS_ORDER if t <= hz]
    reach = (hz, hz - 1)

    def children(way, t):
        return [order.index(c) for c in order if RS_PARENT[c] == t and c <= reach[way]]

    def tile(j):
        t = (order + [0])[(j + 1) // 2]
        return (z + nz + t * (2 * (j % 2) - 1 if j else 1)) % nz

    def tiles(i):
        return (0, 1) if i == 0 else (2 * i - 1, 1 if i == hz else 2)

    def y_send(way, j, i, src, dst, send, recv):
        pltpu.make_async_remote_copy(
            src_ref=src, dst_ref=dst, send_sem=send_sem.at[send], recv_sem=recv.at[i],
            device_id=at(z, y + 1 - 2 * way), device_id_type=MESH).start()

    def ahead(i):
        first, n = tiles(i)
        for k in range(n):
            for way in (0, 1):
                src = g.at[tile(first + k), :, pl.ds(quarter + way * half, half)]
                y_send(way, first + k, i, src, ain.at[way, first + k], 0, a_rsem)

    def direct(i):
        first, n = tiles(i)
        for k in range(n):
            for way in (0, 1):
                src = g.at[tile(first + k), :, pl.ds(2 * way * quarter, quarter)]
                y_send(way, first + k, i, src, bin_.at[way, first + k], 1, b_rsem)

    def arrived(i, ref, sem):
        first, n = tiles(i)
        piece = ref.at[:, pl.ds(first, n)]
        pltpu.make_async_copy(piece, piece, sem.at[i]).wait()

    def relay(i):
        arrived(i, ain, a_rsem)
        first, n = tiles(i)
        for k in range(n):
            for way in (0, 1):
                y_send(way, first + k, i, ain.at[way, first + k], rin.at[way, first + k], 8, r_rsem)

    def z_copy(way, i, h):
        hop = order[i] - RS_PARENT[order[i]]
        return pltpu.make_async_remote_copy(
            src_ref=zout.at[way, i, h], dst_ref=zin.at[way, i, h],
            send_sem=send_sem.at[2 + 7 * way], recv_sem=z_rsem.at[way, i, h],
            device_id=at(z + (1 - 2 * way) * hop, y), device_id_type=MESH)

    def add_arrived(value, way, t, h):
        for i in children(way, t):
            z_copy(way, i, h).wait_recv()
            value = value + zin[way, i, h]
        return value

    def y_sum(j, h):
        cols = pl.ds(h * half, half)
        own = g[tile(j), :, pl.ds(3 * quarter + h * half, half)].astype(jnp.float32)
        left = bin_[0, j, :, cols].astype(jnp.float32)
        right = bin_[1, j, :, cols].astype(jnp.float32)
        far = rin[h, j].astype(jnp.float32)
        return (own + left) + (right + far)

    def step(i):
        if i < ROUNDS:
            round_(i)
        if i + LEAD <= hz:
            relay(i + LEAD)
        if i + 2 + LEAD <= hz:
            ahead(i + 2 + LEAD)
        if i + 2 <= hz:
            direct(i + 2)
        arrived(i, bin_, b_rsem)
        arrived(i, rin, r_rsem)
        for h in (0, 1):
            for way in (0, 1) if i else (0,):
                zout[way, i, h] = add_arrived(y_sum(tiles(i)[0] + way, h), way, order[i], h)
                z_copy(way, i, h).start()

    for way in (0, 1):
        pltpu.make_async_remote_copy(
            src_ref=states_ref, dst_ref=near.at[way], send_sem=send_sem.at[11], recv_sem=near_rsem.at[0],
            device_id=at(z + 1 - 2 * way, y), device_id_type=MESH).start()

    def give_states():
        pltpu.make_async_copy(near, near, near_rsem.at[0]).wait()
        for i in range(1, NY):
            yy = (y + i) % NY
            for src, dst, send in (
                (states_ref.at[:, :, columns(yy)], t_in.at[0, :, y], 12),
                (near.at[:, :, :, columns(yy)], t_in.at[pl.ds(1, 2), :, y], 13),
            ):
                pltpu.make_async_remote_copy(
                    src_ref=src, dst_ref=dst, send_sem=send_sem.at[send], recv_sem=t_rsem.at[0],
                    device_id=at(z, yy), device_id_type=MESH).start()
        for a in range(3):
            t_in[0, a, y] = states_ref[a, :, columns(y)]
            for way in (0, 1):
                t_in[1 + way, a, y] = near[way, a, :, columns(y)]

    for i in range(LEAD + 1):
        if i <= hz:
            ahead(i)
    direct(0)
    if LEAD + 1 <= hz:
        ahead(LEAD + 1)
    direct(1)

    for i in range(LEAD):
        if i <= hz:
            relay(i)

    for i in range(hz):
        step(i)
    give_states()

    squares = jnp.zeros((8, half), jnp.float32)
    arrived(hz, bin_, b_rsem)
    arrived(hz, rin, r_rsem)
    for h in (0, 1):
        value = y_sum(nz - 1, h)
        for way in (0, 1):
            value = add_arrived(value, way, 0, h)
        total_q[0, :, pl.ds(h * half, half)] = value
        squares = squares + value * value

    norm_out[...] = jnp.sum(jnp.sum(squares.reshape(8, half // 128, 128), axis=1), axis=0, keepdims=True)
    mine = e * NY + y
    n1[mine] = norm_out[...]

    def far_first(n):
        return sorted(range(n), key=lambda i: -min(i, n - i))

    def n1_send(k, i):
        ee = ((e // 2 + k) % (n_e // 2)) * 2 + 1
        pltpu.make_async_remote_copy(
            src_ref=norm_out, dst_ref=n1.at[mine], send_sem=send_sem.at[3], recv_sem=n1_rsem.at[0],
            device_id=(ee, z * NY + (y + i) % NY), device_id_type=MESH).start()

    for k in far_first(n_e // 2):
        for i in far_first(NY):
            if k or i:
                n1_send(k, i)
    pl.when(e % 2 == 0)(lambda: n1_send(0, 0))

    for way in (0, 1):
        pltpu.make_async_remote_copy(
            src_ref=total_q.at[0], dst_ref=total_q.at[1 + way], send_sem=send_sem.at[14], recv_sem=q_rsem.at[0],
            device_id=at(z + 1 - 2 * way, y), device_id_type=MESH).start()
    for k in range(NY):
        s_out[k] = total_q[0, pl.ds(2 * k, 2), :]
    for i in range(1, NY):
        yy = (y + i) % NY
        pltpu.make_async_remote_copy(
            src_ref=s_out.at[yy], dst_ref=s_in.at[y], send_sem=send_sem.at[5], recv_sem=x_rsem.at[0],
            device_id=at(z, yy), device_id_type=MESH).start()
    s_in[y] = s_out[y]

    def wait_rows(ref, n, sem):
        piece = ref.at[pl.ds(0, n)]
        pltpu.make_async_copy(piece, piece, sem).wait()

    def n2_send(i, core):
        pltpu.make_async_remote_copy(
            src_ref=norm2_out, dst_ref=n2.at[z], send_sem=send_sem.at[4], recv_sem=n2_rsem.at[0],
            device_id=(e - 1 + core, ((z + i) % nz) * NY + y), device_id_type=MESH).start()

    @pl.when(e % 2 == 1)
    def _():
        wait_rows(n1, n_e * NY - 1, n1_rsem.at[0])
        norm2_out[...] = jnp.sum(n1[...], axis=0)
        n2[z] = norm2_out[...]
        for i in far_first(nz):
            n2_send(i, 0)
            if i:
                n2_send(i, 1)

    s_rest, t_rest, q_rest = s_in.at[pl.ds(0, NY - 1)], t_in.at[:, :, pl.ds(0, NY - 1)], total_q.at[pl.ds(1, 2)]
    for ref, sem in ((s_rest, x_rsem), (t_rest, t_rsem), (q_rest, q_rsem)):
        pltpu.make_async_copy(ref, ref, sem.at[0]).wait()

    pl.when(e % 2 == 1)(lambda: wait_rows(n2, nz - 1, n2_rsem.at[0]))
    pl.when(e % 2 == 0)(lambda: wait_rows(n2, nz, n2_rsem.at[0]))
    norm = jnp.sqrt(jnp.sum(jnp.sum(n2[...], axis=0), axis=1, keepdims=True))
    clip = 1.0 / jnp.maximum(norm, 1.0)

    def update(c, carry):
        states = [jnp.concatenate([t_in[c, a, k] for k in range(NY)], axis=0) for a in range(3)]
        new = adam(clip, total_q[c], *states)[0]
        w_ref[(z + nz + c // 2 - c % 2) % nz, :, columns(y)] = new.astype(jnp.bfloat16)
        return carry

    lax.fori_loop(0, 3, update, 0)

    def az_copy(way, t, hop):
        sign = 1 - 2 * way
        piece = w_ref.at[(z - sign * (t - hop) + nz) % nz, :, columns(y)]
        return pltpu.make_async_remote_copy(
            src_ref=piece, dst_ref=piece, send_sem=send_sem.at[6], recv_sem=z_rsem.at[way, t - 1, 0],
            device_id=at(z + sign * hop, y), device_id_type=MESH)

    def diagonal(way, t, hop):
        sign = 1 - 2 * way
        piece = w_ref.at[(z - sign * (t - hop) + nz) % nz, :, columns(y)]
        j = 2 * t - 1 + way
        for i in (1, 3, 2):
            pltpu.make_async_remote_copy(
                src_ref=piece, dst_ref=piece, send_sem=send_sem.at[7 if i != 2 else 10],
                recv_sem=y_rsem.at[j] if i != 2 else w_rsem.at[0],
                device_id=at(z + sign * hop, y + i), device_id_type=MESH).start()

    def az_pass(way, t):
        far = [c for c in PARENT if PARENT[c] == t and c <= reach[way]]
        if t == 6:
            far = far[::-1]
        for child in far:
            if child in DIAGONAL:
                diagonal(way, child, child - t)
            az_copy(way, child, child - t).start()

    def ag_tile(j):
        t = (j + 1) // 2
        sign = 1 - 2 * (j % 2)
        return (z + nz + sign * t) % nz

    def ay_copy(way, j, forward):
        yy = y if forward else (y - 1 + 2 * way + NY) % NY
        piece = w_ref.at[ag_tile(j), :, columns(yy)]
        return pltpu.make_async_remote_copy(
            src_ref=piece, dst_ref=piece, send_sem=send_sem.at[7], recv_sem=y_rsem.at[j],
            device_id=at(z, y + 1 - 2 * way), device_id_type=MESH)

    def ar_copy(way, j, forward):
        q = ((y - 1 + 2 * way + NY) if forward else (y + 2)) % NY
        piece = w_ref.at[ag_tile(j), :, pl.ds(pl.multiple_of(q * quarter + way * half, 128), half)]
        return pltpu.make_async_remote_copy(
            src_ref=piece, dst_ref=piece, send_sem=send_sem.at[10], recv_sem=w_rsem.at[0],
            device_id=at(z, y + 1 - 2 * way), device_id_type=MESH)

    def y_out(j):
        for way in (0, 1):
            ay_copy(way, j, True).start()

    two = w_ref.at[pl.ds(0, 2), :, pl.ds(0, quarter)]

    def y_relay(j):
        pltpu.make_async_copy(two, two, y_rsem.at[j]).wait()
        for way in (0, 1):
            ar_copy(way, j, True).start()

    for way in (0, 1):
        az_pass(way, 1)
    for j in range(3):
        y_out(j)

    for k in range(NY):
        cols = pl.ds(k * quarter, quarter)
        got = adam(clip, s_in[k], *[states_ref[a, :, cols] for a in range(3)])
        for a, value in enumerate(got):
            outs[a, :, cols] = value

    waiting, leaves = [[0, 1, 2]], []
    for t in [t for t in PARENT if t <= hz]:
        here = []
        for way in (0, 1):
            if t > reach[way]:
                continue
            if t in DIAGONAL:
                leaves.append((way, t))
                continue
            az_copy(way, t, t - PARENT[t]).wait_recv()
            az_pass(way, t)
            here.append(2 * t - 1 + way)
            y_out(here[-1])
        if here:
            waiting.append(here)
            if len(waiting) > AG_LAG:
                for j in waiting.pop(0):
                    y_relay(j)
    for j in sum(waiting, []):
        y_relay(j)
    for way, t in leaves:
        az_copy(way, t, t - PARENT[t]).wait_recv()
        pltpu.make_async_copy(two, two, y_rsem.at[2 * t - 1 + way]).wait()

    relayed = w_ref.at[:, :, pl.ds(0, quarter)]
    pltpu.make_async_copy(relayed, relayed, w_rsem.at[0]).wait()
    sent = (
        (0, ain), (1, bin_), (8, rin), (2, zout.at[0]), (9, zout.at[1, pl.ds(1, hz - 1)]), (5, s_rest), (11, near), (12, t_in.at[0, :, pl.ds(0, NY - 1)]),
        (13, t_in.at[pl.ds(1, 2), :, pl.ds(0, NY - 1)]), (14, q_rest),
        (6, w_ref.at[pl.ds(0, nz - 3), :, pl.ds(0, quarter)]), (7, w_ref.at[:, :, pl.ds(0, 2 * quarter)]), (10, relayed),
    )
    wait_rows(n1, n_e * NY // 2 - 1, send_sem.at[3])
    pl.when(e % 2 == 0)(lambda: wait_rows(n1, 1, send_sem.at[3]))
    pl.when(e % 2 == 1)(lambda: wait_rows(n1, 2 * nz - 1, send_sem.at[4]))
    for i, ref in sent:
        pltpu.make_async_copy(ref, ref, send_sem.at[i]).wait()


def emit(outs, w, *refs):
    sem = refs[5]
    copies = [pltpu.make_async_copy(w, refs[4], sem.at[4])]
    copies += [pltpu.make_async_copy(outs.at[a], refs[a], sem.at[a]) for a in range(4)]
    for copy in copies:
        copy.start()
    for copy in copies:
        copy.wait()


def solution(mesh):
    n_e = mesh.shape["expert"]
    nz = mesh.shape["dp"] // NY

    def step(grads, master, first, second):
        rows, width = grads.shape[2:]
        quarter = width // NY
        half = quarter // 2
        own = master.shape[1:]
        g = grads.reshape(nz, 8, width)
        hz = nz // 2
        f32, bf16 = jnp.float32, jnp.bfloat16
        dma = pltpu.SemaphoreType.DMA
        hbm = pl.BlockSpec(memory_space=pltpu.HBM)
        vmem = pl.BlockSpec(memory_space=pltpu.VMEM)
        out = pl.pallas_call(
            functools.partial(kernel, n_e, nz, quarter),
            out_shape=[jax.ShapeDtypeStruct((4,) + own, f32), jax.ShapeDtypeStruct((nz, 8, width), bf16)],
            in_specs=[hbm, vmem],
            out_specs=[vmem] * 2,
            scratch_shapes=[
                pltpu.VMEM((nz, 8, width), bf16),
                pltpu.VMEM((2, nz, 8, half), bf16),
                pltpu.VMEM((2, nz, 8, quarter), bf16),
                pltpu.VMEM((2, nz, 8, half), bf16),
                pltpu.VMEM((2, hz, 2, 8, half), f32),
                pltpu.VMEM((2, hz, 2, 8, half), f32),
                pltpu.VMEM((3, 8, quarter), f32),
                pltpu.VMEM((2, 3) + own, f32),
                pltpu.VMEM((NY, 2, quarter), f32),
                pltpu.VMEM((NY, 2, quarter), f32),
                pltpu.VMEM((3, 3, NY, 2, quarter), f32),
                pltpu.VMEM((1, 128), f32),
                pltpu.VMEM((n_e * NY, 1, 128), f32),
                pltpu.VMEM((1, 128), f32),
                pltpu.VMEM((nz, 1, 128), f32),
                dma((1,)), dma((15,)), dma((hz + 1,)), dma((hz + 1,)), dma((hz + 1,)), dma((nz,)), dma((2, hz, 2)), *[dma((1,))] * 7, pltpu.SemaphoreType.REGULAR((ROUNDS,)),
            ],
            compiler_params=pltpu.CompilerParams(collective_id=0, has_side_effects=True, vmem_limit_bytes=VMEM_LIMIT),
        )(g, jnp.concatenate([master, first, second], axis=0))
        o_master, o_first, o_second, o_direction, w = pl.pallas_call(
            emit,
            out_shape=[jax.ShapeDtypeStruct(own, f32)] * 4 + [jax.ShapeDtypeStruct((nz, 8, width), bf16)],
            in_specs=[vmem] * 2,
            out_specs=[hbm] * 5,
            scratch_shapes=[dma((5,))],
            compiler_params=pltpu.CompilerParams(vmem_limit_bytes=VMEM_LIMIT),
        )(*out)
        f = lambda a: a.reshape((1,) + own)
        return f(o_master), f(o_first), f(o_second), f(o_direction), w.reshape(1, rows, width)

    rows_spec = P("expert", "dp", None)
    return jax.shard_map(
        step,
        mesh=mesh,
        in_specs=(P("expert", "dp", None, None), rows_spec, rows_spec, rows_spec),
        out_specs=(rows_spec, rows_spec, rows_spec, rows_spec, P("expert", None, None)),
        check_vma=False,
    )
```

```python
import functools

import jax
import jax.numpy as jnp
from jax import lax
from jax.experimental import pallas as pl
from jax.experimental.pallas import tpu as pltpu
from jax.sharding import PartitionSpec as P

STEP = 10
NY = 4
LEAD = 1
RS_ORDER = (8, 7, 5, 6, 4, 2, 3, 1)
RS_PARENT = {8: 6, 7: 6, 6: 3, 5: 3, 4: 3, 3: 0, 2: 0, 1: 0}
ROUNDS = 4
AG_LAG = 2
DIAGONAL = (7, 8)
PARENT = {2: 1, 3: 1, 4: 1, 5: 4, 6: 4, 7: 6, 8: 6}
VMEM_LIMIT = 52 * 1024 * 1024
MESH = pl.DeviceIdType.MESH


def adam(clip, summed, master, first, second):
    clipped = clip * summed
    new_first = 0.9 * first + 0.1 * clipped
    new_second = 0.95 * second + 0.05 * (clipped * clipped)
    first_fix = 1.0 - 0.9**STEP
    second_fix = 1.0 - 0.95**STEP
    direction = new_first / first_fix / (jnp.sqrt(new_second / second_fix) + 1e-08)
    new_master = master - 0.001 * (direction + 0.1 * master)
    return new_master, new_first, new_second, direction


def kernel(
    n_e, nz, quarter,
    g_hbm, states_ref,
    outs, w_ref,
    g, ain, bin_, rin, zin, zout, total_q, near, s_out, s_in, t_in, norm_out, n1, norm2_out, n2,
    load_sem, send_sem, y_rsem, r_rsem, z_rsem, w_rsem, x_rsem, t_rsem, near_rsem, q_rsem, n1_rsem, n2_rsem, met,
):
    half = quarter // 2
    hz = nz // 2
    a_rsem, b_rsem = y_rsem.at[pl.ds(0, hz + 1)], y_rsem.at[pl.ds(hz + 1, hz + 1)]
    e = lax.axis_index("expert")
    d = lax.axis_index("dp")
    z = d // NY
    y = d % NY

    def at(zz, yy):
        return (e, ((zz + nz) % nz) * NY + (yy + NY) % NY)

    def columns(q):
        return pl.ds(pl.multiple_of(q * quarter, 128), quarter)

    for i in range(NY):
        pltpu.make_async_copy(
            g_hbm.at[:, :, columns((y + 1 + i) % NY)], g.at[:, :, pl.ds(i * quarter, quarter)], load_sem.at[0]).start()

    def other(ee):
        return ((ee + n_e) % n_e, d)

    neighbours = [at(z + 1, y), at(z - 1, y), at(z, y + 1), at(z, y - 1), other(e + 1 - 2 * (e % 2))]
    if n_e > 2:
        neighbours += [other(e + 2), other(e - 2)]

    def greet(sem):
        for device in neighbours:
            pl.semaphore_signal(sem, inc=1, device_id=device, device_id_type=MESH)

    barrier = pltpu.get_barrier_semaphore()
    greet(barrier)
    pl.semaphore_wait(barrier, len(neighbours))

    def round_(r):
        pl.semaphore_wait(met.at[r], len(neighbours))
        if r + 1 < ROUNDS:
            greet(met.at[r + 1])

    greet(met.at[0])

    pltpu.make_async_copy(g, g, load_sem.at[0]).wait()

    order = [t for t in RS_ORDER if t <= hz]
    reach = (hz, hz - 1)

    def children(way, t):
        return [order.index(c) for c in order if RS_PARENT[c] == t and c <= reach[way]]

    def tile(j):
        t = (order + [0])[(j + 1) // 2]
        return (z + nz + t * (2 * (j % 2) - 1 if j else 1)) % nz

    def tiles(i):
        return (0, 1) if i == 0 else (2 * i - 1, 1 if i == hz else 2)

    def y_send(way, j, i, src, dst, send, recv):
        pltpu.make_async_remote_copy(
            src_ref=src, dst_ref=dst, send_sem=send_sem.at[send], recv_sem=recv.at[i],
            device_id=at(z, y + 1 - 2 * way), device_id_type=MESH).start()

    def ahead(i):
        first, n = tiles(i)
        for k in range(n):
            for way in (0, 1):
                src = g.at[tile(first + k), :, pl.ds(quarter + way * half, half)]
                y_send(way, first + k, i, src, ain.at[way, first + k], 0, a_rsem)

    def direct(i):
        first, n = tiles(i)
        for k in range(n):
            for way in (0, 1):
                src = g.at[tile(first + k), :, pl.ds(2 * way * quarter, quarter)]
                y_send(way, first + k, i, src, bin_.at[way, first + k], 0, b_rsem)

    def arrived(i, ref, sem):
        first, n = tiles(i)
        piece = ref.at[:, pl.ds(first, n)]
        pltpu.make_async_copy(piece, piece, sem.at[i]).wait()

    def relay(i):
        arrived(i, ain, a_rsem)
        first, n = tiles(i)
        for k in range(n):
            for way in (0, 1):
                y_send(way, first + k, i, ain.at[way, first + k], rin.at[way, first + k], 0, r_rsem)

    def z_copy(way, i, h):
        hop = order[i] - RS_PARENT[order[i]]
        return pltpu.make_async_remote_copy(
            src_ref=zout.at[way, i, h], dst_ref=zin.at[way, i, h],
            send_sem=send_sem.at[2 + 7 * way], recv_sem=z_rsem.at[way, i, h],
            device_id=at(z + (1 - 2 * way) * hop, y), device_id_type=MESH)

    def add_arrived(value, way, t, h):
        for i in children(way, t):
            z_copy(way, i, h).wait_recv()
            value = value + zin[way, i, h]
        return value

    def y_sum(j, h):
        cols = pl.ds(h * half, half)
        own = g[tile(j), :, pl.ds(3 * quarter + h * half, half)].astype(jnp.float32)
        left = bin_[0, j, :, cols].astype(jnp.float32)
        right = bin_[1, j, :, cols].astype(jnp.float32)
        far = rin[h, j].astype(jnp.float32)
        return (own + left) + (right + far)

    def step(i):
        if i < ROUNDS:
            round_(i)
        if i + LEAD <= hz:
            relay(i + LEAD)
        if i + 2 + LEAD <= hz:
            ahead(i + 2 + LEAD)
        if i + 2 <= hz:
            direct(i + 2)
        arrived(i, bin_, b_rsem)
        arrived(i, rin, r_rsem)
        for h in (0, 1):
            for way in (0, 1) if i else (0,):
                zout[way, i, h] = add_arrived(y_sum(tiles(i)[0] + way, h), way, order[i], h)
                z_copy(way, i, h).start()

    for way in (0, 1):
        pltpu.make_async_remote_copy(
            src_ref=states_ref, dst_ref=near.at[way], send_sem=send_sem.at[8], recv_sem=near_rsem.at[0],
            device_id=at(z + 1 - 2 * way, y), device_id_type=MESH).start()

    def give_states():
        pltpu.make_async_copy(near, near, near_rsem.at[0]).wait()
        for i in range(1, NY):
            yy = (y + i) % NY
            for src, dst, send in (
                (states_ref.at[:, :, columns(yy)], t_in.at[0, :, y], 1),
                (near.at[:, :, :, columns(yy)], t_in.at[pl.ds(1, 2), :, y], 1),
            ):
                pltpu.make_async_remote_copy(
                    src_ref=src, dst_ref=dst, send_sem=send_sem.at[send], recv_sem=t_rsem.at[0],
                    device_id=at(z, yy), device_id_type=MESH).start()
        for a in range(3):
            t_in[0, a, y] = states_ref[a, :, columns(y)]
            for way in (0, 1):
                t_in[1 + way, a, y] = near[way, a, :, columns(y)]

    for i in range(LEAD + 1):
        if i <= hz:
            ahead(i)
    direct(0)
    if LEAD + 1 <= hz:
        ahead(LEAD + 1)
    direct(1)

    for i in range(LEAD):
        if i <= hz:
            relay(i)

    for i in range(hz):
        step(i)
    give_states()

    squares = jnp.zeros((8, half), jnp.float32)
    arrived(hz, bin_, b_rsem)
    arrived(hz, rin, r_rsem)
    for h in (0, 1):
        value = y_sum(nz - 1, h)
        for way in (0, 1):
            value = add_arrived(value, way, 0, h)
        total_q[0, :, pl.ds(h * half, half)] = value
        squares = squares + value * value

    norm_out[...] = jnp.sum(jnp.sum(squares.reshape(8, half // 128, 128), axis=1), axis=0, keepdims=True)
    mine = e * NY + y
    n1[mine] = norm_out[...]

    def far_first(n):
        return sorted(range(n), key=lambda i: -min(i, n - i))

    def n1_send(k, i):
        ee = ((e // 2 + k) % (n_e // 2)) * 2 + 1
        pltpu.make_async_remote_copy(
            src_ref=norm_out, dst_ref=n1.at[mine], send_sem=send_sem.at[3], recv_sem=n1_rsem.at[0],
            device_id=(ee, z * NY + (y + i) % NY), device_id_type=MESH).start()

    for k in far_first(n_e // 2):
        for i in far_first(NY):
            if k or i:
                n1_send(k, i)
    pl.when(e % 2 == 0)(lambda: n1_send(0, 0))

    for way in (0, 1):
        pltpu.make_async_remote_copy(
            src_ref=total_q.at[0], dst_ref=total_q.at[1 + way], send_sem=send_sem.at[10], recv_sem=q_rsem.at[0],
            device_id=at(z + 1 - 2 * way, y), device_id_type=MESH).start()
    for k in range(NY):
        s_out[k] = total_q[0, pl.ds(2 * k, 2), :]
    for i in range(1, NY):
        yy = (y + i) % NY
        pltpu.make_async_remote_copy(
            src_ref=s_out.at[yy], dst_ref=s_in.at[y], send_sem=send_sem.at[5], recv_sem=x_rsem.at[0],
            device_id=at(z, yy), device_id_type=MESH).start()
    s_in[y] = s_out[y]

    def wait_rows(ref, n, sem):
        piece = ref.at[pl.ds(0, n)]
        pltpu.make_async_copy(piece, piece, sem).wait()

    def n2_send(i, core):
        pltpu.make_async_remote_copy(
            src_ref=norm2_out, dst_ref=n2.at[z], send_sem=send_sem.at[4], recv_sem=n2_rsem.at[0],
            device_id=(e - 1 + core, ((z + i) % nz) * NY + y), device_id_type=MESH).start()

    @pl.when(e % 2 == 1)
    def _():
        wait_rows(n1, n_e * NY - 1, n1_rsem.at[0])
        norm2_out[...] = jnp.sum(n1[...], axis=0)
        n2[z] = norm2_out[...]
        for i in far_first(nz):
            n2_send(i, 0)
            if i:
                n2_send(i, 1)

    s_rest, t_rest, q_rest = s_in.at[pl.ds(0, NY - 1)], t_in.at[:, :, pl.ds(0, NY - 1)], total_q.at[pl.ds(1, 2)]
    for ref, sem in ((s_rest, x_rsem), (t_rest, t_rsem), (q_rest, q_rsem)):
        pltpu.make_async_copy(ref, ref, sem.at[0]).wait()

    pl.when(e % 2 == 1)(lambda: wait_rows(n2, nz - 1, n2_rsem.at[0]))
    pl.when(e % 2 == 0)(lambda: wait_rows(n2, nz, n2_rsem.at[0]))
    norm = jnp.sqrt(jnp.sum(jnp.sum(n2[...], axis=0), axis=1, keepdims=True))
    clip = 1.0 / jnp.maximum(norm, 1.0)

    def update(c, carry):
        states = [jnp.concatenate([t_in[c, a, k] for k in range(NY)], axis=0) for a in range(3)]
        new = adam(clip, total_q[c], *states)[0]
        w_ref[(z + nz + c // 2 - c % 2) % nz, :, columns(y)] = new.astype(jnp.bfloat16)
        return carry

    lax.fori_loop(0, 3, update, 0)

    def az_copy(way, t, hop):
        sign = 1 - 2 * way
        piece = w_ref.at[(z - sign * (t - hop) + nz) % nz, :, columns(y)]
        return pltpu.make_async_remote_copy(
            src_ref=piece, dst_ref=piece, send_sem=send_sem.at[6], recv_sem=z_rsem.at[way, t - 1, 0],
            device_id=at(z + sign * hop, y), device_id_type=MESH)

    def diagonal(way, t, hop):
        sign = 1 - 2 * way
        piece = w_ref.at[(z - sign * (t - hop) + nz) % nz, :, columns(y)]
        j = 2 * t - 1 + way
        for i in (1, 3, 2):
            pltpu.make_async_remote_copy(
                src_ref=piece, dst_ref=piece, send_sem=send_sem.at[7],
                recv_sem=y_rsem.at[j] if i != 2 else w_rsem.at[0],
                device_id=at(z + sign * hop, y + i), device_id_type=MESH).start()

    def az_pass(way, t):
        far = [c for c in PARENT if PARENT[c] == t and c <= reach[way]]
        if t == 6:
            far = far[::-1]
        for child in far:
            if child in DIAGONAL:
                diagonal(way, child, child - t)
            az_copy(way, child, child - t).start()

    def ag_tile(j):
        t = (j + 1) // 2
        sign = 1 - 2 * (j % 2)
        return (z + nz + sign * t) % nz

    def ay_copy(way, j, forward):
        yy = y if forward else (y - 1 + 2 * way + NY) % NY
        piece = w_ref.at[ag_tile(j), :, columns(yy)]
        return pltpu.make_async_remote_copy(
            src_ref=piece, dst_ref=piece, send_sem=send_sem.at[7], recv_sem=y_rsem.at[j],
            device_id=at(z, y + 1 - 2 * way), device_id_type=MESH)

    def ar_copy(way, j, forward):
        q = ((y - 1 + 2 * way + NY) if forward else (y + 2)) % NY
        piece = w_ref.at[ag_tile(j), :, pl.ds(pl.multiple_of(q * quarter + way * half, 128), half)]
        return pltpu.make_async_remote_copy(
            src_ref=piece, dst_ref=piece, send_sem=send_sem.at[7], recv_sem=w_rsem.at[0],
            device_id=at(z, y + 1 - 2 * way), device_id_type=MESH)

    def y_out(j):
        for way in (0, 1):
            ay_copy(way, j, True).start()

    two = w_ref.at[pl.ds(0, 2), :, pl.ds(0, quarter)]

    def y_relay(j):
        pltpu.make_async_copy(two, two, y_rsem.at[j]).wait()
        for way in (0, 1):
            ar_copy(way, j, True).start()

    for way in (0, 1):
        az_pass(way, 1)
    for j in range(3):
        y_out(j)

    for k in range(NY):
        cols = pl.ds(k * quarter, quarter)
        got = adam(clip, s_in[k], *[states_ref[a, :, cols] for a in range(3)])
        for a, value in enumerate(got):
            outs[a, :, cols] = value

    waiting, leaves = [[0, 1, 2]], []
    for t in [t for t in PARENT if t <= hz]:
        here = []
        for way in (0, 1):
            if t > reach[way]:
                continue
            if t in DIAGONAL:
                leaves.append((way, t))
                continue
            az_copy(way, t, t - PARENT[t]).wait_recv()
            az_pass(way, t)
            here.append(2 * t - 1 + way)
            y_out(here[-1])
        if here:
            waiting.append(here)
            if len(waiting) > AG_LAG:
                for j in waiting.pop(0):
                    y_relay(j)
    for j in sum(waiting, []):
        y_relay(j)
    for way, t in leaves:
        az_copy(way, t, t - PARENT[t]).wait_recv()
        pltpu.make_async_copy(two, two, y_rsem.at[2 * t - 1 + way]).wait()

    relayed = w_ref.at[:, :, pl.ds(0, quarter)]
    pltpu.make_async_copy(relayed, relayed, w_rsem.at[0]).wait()
    sent = (
        (0, g), (1, t_rest), (2, zout.at[0]), (9, zout.at[1, pl.ds(1, hz - 1)]), (5, s_rest),
        (6, w_ref.at[pl.ds(0, nz - 3), :, pl.ds(0, quarter)]), (7, w_ref.at[:, :, pl.ds(0, 3 * quarter)]), (8, near), (10, q_rest),
    )
    wait_rows(n1, n_e * NY // 2 - 1, send_sem.at[3])
    pl.when(e % 2 == 0)(lambda: wait_rows(n1, 1, send_sem.at[3]))
    pl.when(e % 2 == 1)(lambda: wait_rows(n1, 2 * nz - 1, send_sem.at[4]))
    for i, ref in sent:
        pltpu.make_async_copy(ref, ref, send_sem.at[i]).wait()


def emit(outs, w, *refs):
    sem = refs[5]
    copies = [pltpu.make_async_copy(w, refs[4], sem.at[4])]
    copies += [pltpu.make_async_copy(outs.at[a], refs[a], sem.at[a]) for a in range(4)]
    for copy in copies:
        copy.start()
    for copy in copies:
        copy.wait()


def solution(mesh):
    n_e = mesh.shape["expert"]
    nz = mesh.shape["dp"] // NY

    def step(grads, master, first, second):
        rows, width = grads.shape[2:]
        quarter = width // NY
        half = quarter // 2
        own = master.shape[1:]
        g = grads.reshape(nz, 8, width)
        hz = nz // 2
        f32, bf16 = jnp.float32, jnp.bfloat16
        dma = pltpu.SemaphoreType.DMA
        hbm = pl.BlockSpec(memory_space=pltpu.HBM)
        vmem = pl.BlockSpec(memory_space=pltpu.VMEM)
        out = pl.pallas_call(
            functools.partial(kernel, n_e, nz, quarter),
            out_shape=[jax.ShapeDtypeStruct((4,) + own, f32), jax.ShapeDtypeStruct((nz, 8, width), bf16)],
            in_specs=[hbm, vmem],
            out_specs=[vmem] * 2,
            scratch_shapes=[
                pltpu.VMEM((nz, 8, width), bf16),
                pltpu.VMEM((2, nz, 8, half), bf16),
                pltpu.VMEM((2, nz, 8, quarter), bf16),
                pltpu.VMEM((2, nz, 8, half), bf16),
                pltpu.VMEM((2, hz, 2, 8, half), f32),
                pltpu.VMEM((2, hz, 2, 8, half), f32),
                pltpu.VMEM((3, 8, quarter), f32),
                pltpu.VMEM((2, 3) + own, f32),
                pltpu.VMEM((NY, 2, quarter), f32),
                pltpu.VMEM((NY, 2, quarter), f32),
                pltpu.VMEM((3, 3, NY, 2, quarter), f32),
                pltpu.VMEM((1, 128), f32),
                pltpu.VMEM((n_e * NY, 1, 128), f32),
                pltpu.VMEM((1, 128), f32),
                pltpu.VMEM((nz, 1, 128), f32),
                dma((1,)), dma((11,)), dma((2 * hz + 2,)), dma((hz + 1,)), dma((2, hz, 2)), *[dma((1,))] * 7, pltpu.SemaphoreType.REGULAR((ROUNDS,)),
            ],
            compiler_params=pltpu.CompilerParams(collective_id=0, has_side_effects=True, vmem_limit_bytes=VMEM_LIMIT),
        )(g, jnp.concatenate([master, first, second], axis=0))
        o_master, o_first, o_second, o_direction, w = pl.pallas_call(
            emit,
            out_shape=[jax.ShapeDtypeStruct(own, f32)] * 4 + [jax.ShapeDtypeStruct((nz, 8, width), bf16)],
            in_specs=[vmem] * 2,
            out_specs=[hbm] * 5,
            scratch_shapes=[dma((5,))],
            compiler_params=pltpu.CompilerParams(vmem_limit_bytes=VMEM_LIMIT),
        )(*out)
        f = lambda a: a.reshape((1,) + own)
        return f(o_master), f(o_first), f(o_second), f(o_direction), w.reshape(1, rows, width)

    rows_spec = P("expert", "dp", None)
    return jax.shard_map(
        step,
        mesh=mesh,
        in_specs=(P("expert", "dp", None, None), rows_spec, rows_spec, rows_spec),
        out_specs=(rows_spec, rows_spec, rows_spec, rows_spec, P("expert", None, None)),
        check_vma=False,
    )
```
